256 devices in a mesh: section: 8 (over z_hi, x), dp: 32 (over y, z_lo, core).
Axes of the slice: x: 4, y: 4, z: 8 (z_hi: 2, z_lo: 4; z = z_hi * 4 + z_lo), core: 2. Of those that a mesh axis runs over, the one named last changes fastest.
Arguments:
- inputs: bfloat16 [4, 4096, 1536], P(None, 'dp'), may hold values from -6 to 6
- out_grad: bfloat16 [4, 4096, 1536], P(None, 'dp'), may hold values from -0.09375 to 0.09375
- guide_bin: int32 [4, 1], replicated, may hold values from 0 to 31
- time_step: int32 [4, 1], replicated, may hold values from 0 to 999
- guide_table: bfloat16 [32, 4608], replicated, may hold values from -3 to 3
- section_table: float32 [8, 3, 1536], P('section'), may hold values from -3 to 3
- value_weight: bfloat16 [8, 1536, 1536], P('section'), may hold values from -0.15625 to 0.15625
- proj_weight: bfloat16 [8, 1536, 1536], P('section'), may hold values from -0.15625 to 0.15625
Outputs:
- value_grad: float32 [8, 1536, 1536], P('section', 'dp')
- proj_grad: float32 [8, 1536, 1536], P('section', 'dp')
- table_grad: float32 [8, 3, 1536], P('section', None, 'dp')
The draws below stay inside these ranges and needn't reach their ends.
All inputs are finite; a program needn't handle non-finite values.
Results may differ from the reference program's by a relative error of at most 0.017.
Values may be sent and summed in bfloat16 or wider, within the bound.
A program may use at most 128 MiB of HBM per device.

```python
import math
import jax
import jax.numpy as jnp
from jax import lax

D = 1536
H = 1536
MICRO = 4
BINS = 32
STEPS = 1000
TOKENS = 4096
SAMPLES = 1
BLOCKS = 8


def plant(drawn, own_key, least, high):
    dims = drawn.shape
    spot = [jax.random.randint(jax.random.fold_in(own_key, axis), (), 0, dims[axis]) for axis in range(len(dims))]
    drawn = drawn.at[tuple(spot)].set(least)
    longest = dims.index(max(dims))
    spot[longest] = (spot[longest] + 1) % dims[longest]
    return drawn.at[tuple(spot)].set(high)


def levels(key, extent, cuts, least, top_value):
    def one(axis_at, blocks):
        steps = jax.random.uniform(jax.random.fold_in(jax.random.fold_in(key, 6), axis_at), (blocks,), jnp.float32, least / len(cuts), top_value / len(cuts))
        return jnp.repeat(jnp.exp(steps), extent[axis_at] // blocks).reshape((-1,) + (1,) * (len(extent) - axis_at - 1))

    factor_of = one(*cuts[0])
    for cut in cuts[1:]:
        factor_of = factor_of * one(*cut)
    return factor_of


def normal_values(stream_key, extent, deviation, bound, pieces=(), kind=jnp.bfloat16):
    array = jax.random.normal(stream_key, extent, jnp.float32) * deviation
    if len(pieces) > 0:
        array = levels(stream_key, extent, pieces, -0.22, 0.18) * array
    return jnp.clip(array, min=-bound, max=bound).astype(kind)


def setup_inputs(seed: int = 0) -> dict:
    arg_keys = jax.random.split(jax.random.key(seed), 9)
    inputs = normal_values(arg_keys[0], (MICRO, TOKENS, D), 1.0, 6.0, ((1, 32),))
    out_grad = normal_values(arg_keys[1], (MICRO, TOKENS, D), TOKENS ** -0.5, 0.09375, ((1, 32),))
    guide_bin = plant(jax.random.randint(arg_keys[2], (MICRO, SAMPLES), 0, BINS), jax.random.fold_in(arg_keys[2], 1), 0, BINS - 1).astype(jnp.int32)
    time_step = plant(jax.random.randint(arg_keys[3], (MICRO, SAMPLES), 0, STEPS), jax.random.fold_in(arg_keys[3], 1), 0, STEPS - 1).astype(jnp.int32)
    guide_table = normal_values(arg_keys[4], (BINS, 3 * D), 0.5, 3.0)
    section_table = normal_values(arg_keys[5], (BLOCKS, 3, D), 0.5, 3.0, ((0, 8),), jnp.float32)
    value_weight = normal_values(arg_keys[6], (BLOCKS, D, H), D ** -0.5, 0.15625, ((0, 8),))
    proj_weight = normal_values(arg_keys[7], (BLOCKS, H, D), H ** -0.5, 0.15625, ((0, 8),))
    return {"inputs": inputs, "out_grad": out_grad, "guide_bin": guide_bin, "time_step": time_step, "guide_table": guide_table, "section_table": section_table, "value_weight": value_weight, "proj_weight": proj_weight}


NORM_FLOOR = 0.1

def normalize(hidden):
    centre = lax.optimization_barrier(jnp.mean(hidden, axis=-1, keepdims=True))
    centred = hidden - centre
    spread = lax.optimization_barrier(jnp.mean(centred * centred, axis=-1, keepdims=True))
    inverse = lax.rsqrt(spread + NORM_FLOOR)
    return (centred * inverse, inverse)

def conditions(guide_bin, time_step, guide_table):
    total = guide_table.shape[1]
    half = total // 2
    frequency = jnp.exp(-math.log(10000.0) * jnp.arange(half, dtype=jnp.float32) / half)
    angle = time_step.astype(jnp.float32)[..., None] * frequency
    waves = jnp.concatenate([jnp.sin(angle), jnp.cos(angle)], axis=-1)
    return guide_table.astype(jnp.float32)[guide_bin] + 0.5 * waves

def forward_block(block_in, modulation, value_weight, proj_weight):
    width = block_in.shape[1]
    hidden = block_in.astype(jnp.float32)
    normed, inverse = normalize(hidden)
    shift = modulation[:, :width]
    scale = modulation[:, width:2 * width]
    gate = modulation[:, 2 * width:]
    modulated = (normed * (1.0 + scale) + shift).astype(jnp.bfloat16)
    values = jnp.dot(modulated, value_weight, preferred_element_type=jnp.float32).astype(jnp.bfloat16)
    projected = jnp.dot(values, proj_weight, preferred_element_type=jnp.float32)
    block_out = (hidden + gate * projected).astype(jnp.bfloat16)
    return (block_out, modulated, values, projected)

def backward_block(block_in, modulated, values, projected, upstream, modulation, value_weight, proj_weight):
    width = block_in.shape[1]
    hidden = block_in.astype(jnp.float32)
    normed, inverse = normalize(hidden)
    scale = modulation[:, width:2 * width]
    gate = modulation[:, 2 * width:]
    grad_up = upstream.astype(jnp.float32)
    grad_proj = (gate * grad_up).astype(jnp.bfloat16)
    part_proj = jnp.dot(values.T, grad_proj, preferred_element_type=jnp.float32)
    grad_values = jnp.dot(grad_proj, proj_weight.T, preferred_element_type=jnp.float32).astype(jnp.bfloat16)
    part_value = jnp.dot(modulated.T, grad_values, preferred_element_type=jnp.float32)
    grad_mod = jnp.dot(grad_values, value_weight.T, preferred_element_type=jnp.float32)
    part_table = jnp.stack([lax.optimization_barrier(jnp.sum(grad_mod, axis=0)), lax.optimization_barrier(jnp.sum(grad_mod * normed, axis=0)), lax.optimization_barrier(jnp.sum(grad_up * projected, axis=0))])
    grad_norm = grad_mod * (1.0 + scale)
    centre_grad = lax.optimization_barrier(jnp.mean(grad_norm, axis=-1, keepdims=True))
    cross = lax.optimization_barrier(jnp.mean(grad_norm * normed, axis=-1, keepdims=True))
    grad_in = grad_up + inverse * (grad_norm - centre_grad - normed * cross)
    return (grad_in.astype(jnp.bfloat16), part_value, part_proj, part_table)

def reference(inputs, out_grad, guide_bin, time_step, guide_table, section_table, value_weight, proj_weight):
    condition = conditions(guide_bin, time_step, guide_table)
    rows_per = TOKENS // SAMPLES
    saved = []
    shared_all = []
    for batch in range(MICRO):
        shared = jnp.repeat(condition[batch], rows_per, axis=0)
        shared_all.append(shared)
        block_in = inputs[batch]
        kept = []
        for block in range(BLOCKS):
            modulation = shared + section_table[block].reshape(-1)
            kept.append(block_in)
            block_in = forward_block(block_in, modulation, value_weight[block], proj_weight[block])[0]
        saved.append(kept)
    value_sums = [jnp.zeros((D, H), jnp.float32) for index in range(BLOCKS)]
    proj_sums = [jnp.zeros((H, D), jnp.float32) for index in range(BLOCKS)]
    table_sums = [jnp.zeros((3, D), jnp.float32) for index in range(BLOCKS)]
    for batch in range(MICRO):
        upstream = out_grad[batch]
        for block in range(BLOCKS - 1, -1, -1):
            modulation = shared_all[batch] + section_table[block].reshape(-1)
            block_in = saved[batch][block]
            block_out, modulated, values, projected = forward_block(block_in, modulation, value_weight[block], proj_weight[block])
            upstream, part_value, part_proj, part_table = backward_block(block_in, modulated, values, projected, upstream, modulation, value_weight[block], proj_weight[block])
            value_sums[block] = value_sums[block] + part_value
            proj_sums[block] = proj_sums[block] + part_proj
            table_sums[block] = table_sums[block] + part_table
    return (jnp.stack(value_sums), jnp.stack(proj_sums), jnp.stack(table_sums))
```

```python
import functools
import math

import jax
import jax.numpy as jnp
from jax import lax
from jax.experimental import pallas as pl
from jax.experimental.pallas import tpu as pltpu
from jax.sharding import Mesh
from jax.sharding import PartitionSpec as P

DP = ("dp_0", "dp_1", "dp_2")
AXES = ("section",) + DP
NORM_FLOOR = 0.1
ROWS = 32
LAG = 3
MESH = pl.DeviceIdType.MESH


def conditions(guide_bin, time_step, guide_table):
    total = guide_table.shape[1]
    half = total // 2
    frequency = jnp.exp(-math.log(10000.0) * jnp.arange(half, dtype=jnp.float32) / half)
    angle = time_step.astype(jnp.float32)[..., None] * frequency
    waves = jnp.concatenate([jnp.sin(angle), jnp.cos(angle)], axis=-1)
    bin_count = guide_table.shape[0]
    onehot = (guide_bin[..., None] == jnp.arange(bin_count, dtype=jnp.int32)).astype(jnp.float32)
    picked = jnp.einsum(
        "msb,bw->msw", onehot, guide_table.astype(jnp.float32), precision=lax.Precision.HIGHEST
    )
    return picked + 0.5 * waves


def dot_plain(left, right):
    return lax.dot_general(
        left, right, (((1,), (0,)), ((), ())), preferred_element_type=jnp.float32
    )


def dot_transposed(left, right):
    return lax.dot_general(
        left, right, (((1,), (1,)), ((), ())), preferred_element_type=jnp.float32
    )


def pipeline_kernel(
    dims,
    inputs_ref,
    out_grad_ref,
    modulation_ref,
    value_ref,
    proj_ref,
    keep_mod,
    keep_val,
    keep_gp,
    keep_gv,
    table_ref,
    x_in,
    g_in,
    x_out,
    g_out,
    keep_norm,
    keep_inv,
    keep_proj,
    table_sum,
    load_sem,
    fwd_send,
    fwd_recv,
    bwd_send,
    bwd_recv,
    mirror_send,
):
    sections, zs, chunks, per_micro, rows = dims
    section = lax.axis_index("section")
    y_at = lax.axis_index("dp_0")
    z_at = lax.axis_index("dp_1")
    core = lax.axis_index("dp_2")
    last = sections - 1
    half = sections // 2
    mirrored = zs - 1 - z_at
    next_z = jnp.where(section == half - 1, mirrored, z_at)
    prev_z = jnp.where(section == half, mirrored, z_at)
    next_id = (jnp.minimum(section + 1, last), y_at, next_z, core)
    prev_id = (jnp.maximum(section - 1, 0), y_at, prev_z, core)
    mirror_id = (section, y_at, mirrored, core)

    def load(c):
        return pltpu.make_async_copy(inputs_ref.at[c], x_in.at[c], load_sem.at[c])

    def send_forward(c):
        return pltpu.make_async_remote_copy(
            src_ref=x_out.at[c],
            dst_ref=x_in.at[c],
            send_sem=fwd_send.at[c],
            recv_sem=fwd_recv.at[c],
            device_id=next_id,
            device_id_type=MESH,
        )

    def send_backward(c):
        return pltpu.make_async_remote_copy(
            src_ref=g_out.at[c],
            dst_ref=g_in.at[c],
            send_sem=bwd_send.at[c],
            recv_sem=bwd_recv.at[c],
            device_id=prev_id,
            device_id_type=MESH,
        )

    def send_mirror(c):
        return pltpu.make_async_remote_copy(
            src_ref=out_grad_ref.at[c],
            dst_ref=g_in.at[c],
            send_sem=mirror_send.at[c],
            recv_sem=bwd_recv.at[c],
            device_id=mirror_id,
            device_id_type=MESH,
        )

    @pl.when(section == 0)
    def _():
        @pl.loop(0, chunks)
        def _(c):
            load(c).start()

    barrier = pltpu.get_barrier_semaphore()

    @pl.when(section < last)
    def _():
        pl.semaphore_signal(barrier, inc=1, device_id=next_id, device_id_type=MESH)

    @pl.when(section > 0)
    def _():
        pl.semaphore_signal(barrier, inc=1, device_id=prev_id, device_id_type=MESH)

    @pl.when(section == last)
    def _():
        pl.semaphore_signal(barrier, inc=1, device_id=mirror_id, device_id_type=MESH)

    pl.semaphore_wait(barrier, jnp.where(section == 0, 1, 2))

    @pl.when(section == last)
    def _():
        @pl.loop(0, chunks)
        def _(c):
            send_mirror(c).start()

    table_sum[...] = jnp.zeros_like(table_sum)

    def forward(c):
        @pl.when(section == 0)
        def _():
            load(c).wait()

        @pl.when(section > 0)
        def _():
            send_forward(c).wait_recv()

        batch = c // per_micro
        hidden = x_in[c].astype(jnp.float32)
        centre = jnp.mean(hidden, axis=-1, keepdims=True)
        centred = hidden - centre
        spread = jnp.mean(centred * centred, axis=-1, keepdims=True)
        inverse = lax.rsqrt(spread + NORM_FLOOR)
        normed = centred * inverse
        shift = modulation_ref[batch, 0:1, :]
        scale = modulation_ref[batch, 1:2, :]
        gate = modulation_ref[batch, 2:3, :]
        modulated = (normed * scale + shift).astype(jnp.bfloat16)
        values = dot_plain(modulated, value_ref[...]).astype(jnp.bfloat16)
        projected = dot_plain(values, proj_ref[...])

        @pl.when(section < last)
        def _():
            x_out[c] = (hidden + gate * projected).astype(jnp.bfloat16)
            send_forward(c).start()

        keep_mod[c] = modulated
        keep_val[c] = values
        keep_norm[c] = normed
        keep_inv[c] = jnp.broadcast_to(inverse, (rows, 128))
        keep_proj[c] = projected

    def backward(c):
        batch = c // per_micro
        scale = modulation_ref[batch, 1:2, :]
        gate = modulation_ref[batch, 2:3, :]
        send_backward(c).wait_recv()
        grad_up = g_in[c].astype(jnp.float32)
        grad_proj = (gate * grad_up).astype(jnp.bfloat16)
        grad_values = dot_transposed(grad_proj, proj_ref[...]).astype(jnp.bfloat16)
        grad_mod = dot_transposed(grad_values, value_ref[...])
        normed = keep_norm[c]

        @pl.when(section > 0)
        def _():
            grad_norm = grad_mod * scale
            centre_grad = jnp.mean(grad_norm, axis=-1, keepdims=True)
            cross = jnp.mean(grad_norm * normed, axis=-1, keepdims=True)
            inverse = keep_inv[c][:, 0:1]
            grad_in = grad_up + inverse * (grad_norm - centre_grad - normed * cross)
            g_out[c] = grad_in.astype(jnp.bfloat16)
            send_backward(c).start()

        keep_gp[c] = grad_proj
        keep_gv[c] = grad_values
        width = grad_mod.shape[1]

        def folded(value):
            return value.reshape(rows // 8, 8, width).sum(axis=0)

        table_sum[0] += folded(grad_mod)
        table_sum[1] += folded(grad_mod * normed)
        table_sum[2] += folded(grad_up * keep_proj[c])

    lag = LAG * (last - section)

    @pl.loop(0, chunks + LAG * last)
    def _(i):
        @pl.when(i < chunks)
        def _():
            forward(i)

        c = i - lag

        @pl.when((c >= 0) & (c < chunks))
        def _():
            backward(c)

    for part in range(3):
        table_ref[part : part + 1, :] = table_sum[part].sum(axis=0, keepdims=True)

    @pl.loop(0, chunks)
    def _(c):
        @pl.when(section < last)
        def _():
            send_forward(c).wait_send()

        @pl.when(section > 0)
        def _():
            send_backward(c).wait_send()

        @pl.when(section == last)
        def _():
            send_mirror(c).wait_send()


def run_pipeline(mesh, inputs, out_grad, modulation, value_weight, proj_weight):
    batches, tok_dev, width = inputs.shape
    value_width = value_weight.shape[1]
    rows = min(ROWS, tok_dev)
    chunks = batches * tok_dev // rows
    sections = mesh.shape["section"]
    dims = (sections, mesh.shape["dp_1"], chunks, tok_dev // rows, rows)
    vmem = pl.BlockSpec(memory_space=pltpu.VMEM)
    hbm = pl.BlockSpec(memory_space=pl.ANY)
    kept = jax.ShapeDtypeStruct((chunks, rows, width), jnp.bfloat16)
    kept_val = jax.ShapeDtypeStruct((chunks, rows, value_width), jnp.bfloat16)
    dma = pltpu.SemaphoreType.DMA((chunks,))
    block = pltpu.VMEM((chunks, rows, width), jnp.bfloat16)
    wide = pltpu.VMEM((chunks, rows, width), jnp.float32)
    outs = pl.pallas_call(
        functools.partial(pipeline_kernel, dims),
        out_shape=(
            kept,
            kept_val,
            kept,
            kept_val,
            jax.ShapeDtypeStruct((3, width), jnp.float32),
        ),
        in_specs=[hbm, hbm, vmem, vmem, vmem],
        out_specs=(vmem,) * 5,
        scratch_shapes=[
            block,
            block,
            block,
            block,
            wide,
            pltpu.VMEM((chunks, rows, 128), jnp.float32),
            wide,
            pltpu.VMEM((3, 8, width), jnp.float32),
            dma,
            dma,
            dma,
            dma,
            dma,
            dma,
        ],
        compiler_params=pltpu.CompilerParams(
            collective_id=0, has_side_effects=True, vmem_limit_bytes=58 * 1024 * 1024
        ),
    )(
        inputs.reshape(chunks, rows, width),
        out_grad.reshape(chunks, rows, width),
        modulation,
        value_weight,
        proj_weight,
    )
    return outs


def split_up(value, dim, peers):
    dims = value.shape
    parts = value.reshape(*dims[:dim], peers, dims[dim] // peers, *dims[dim + 1 :])
    return jnp.moveaxis(parts, dim, 0)


def sum_by_chip(value, chips, core, dim):
    sizes = (lax.axis_size(chips), lax.axis_size(core))
    parts = split_up(value, dim, sizes[0] * sizes[1])
    inside = parts.shape[1:]
    parts = parts.reshape(*sizes, *inside).swapaxes(0, 1).reshape(-1, *inside)
    parts = lax.psum_scatter(parts, core, scatter_dimension=0, tiled=True)
    return lax.psum_scatter(parts, chips, scatter_dimension=0, tiled=True)[0]


def summed_on_arrival(value, axis, dim):
    parts = split_up(value, dim, lax.axis_size(axis))
    arrived = lax.all_to_all(parts, axis, split_axis=0, concat_axis=0, tiled=True)
    return arrived.sum(axis=0)


def contract_rows(left, right):
    left = left.reshape(-1, left.shape[-1])
    right = right.reshape(-1, right.shape[-1])
    return lax.dot_general(
        left, right, (((0,), (0,)), ((), ())), preferred_element_type=jnp.float32
    )


def per_device(
    mesh,
    inputs,
    out_grad,
    guide_bin,
    time_step,
    guide_table,
    section_table,
    value_weight,
    proj_weight,
):
    batches, tok_dev, width = inputs.shape
    assert guide_bin.shape[1] == 1
    condition = conditions(guide_bin, time_step, guide_table)
    modulation = condition[:, 0] + section_table[0].reshape(-1)
    modulation = modulation.reshape(batches, 3, width)
    modulation = modulation + jnp.array([0.0, 1.0, 0.0], jnp.float32)[None, :, None]
    keep_mod, keep_val, keep_gp, keep_gv, table_sum = run_pipeline(
        mesh, inputs, out_grad, modulation, value_weight[0], proj_weight[0]
    )
    value_full = contract_rows(keep_mod, keep_gv).astype(jnp.bfloat16)
    value_part = sum_by_chip(value_full, ("dp_0", "dp_1"), "dp_2", 0)
    proj_full = contract_rows(keep_val, keep_gp).astype(jnp.bfloat16)
    proj_part = sum_by_chip(proj_full, ("dp_0", "dp_1"), "dp_2", 0)
    table_part = summed_on_arrival(table_sum, DP, 1)
    return (
        value_part.astype(jnp.float32)[None],
        proj_part.astype(jnp.float32)[None],
        table_part[None],
    )


def solution(mesh):
    finer = Mesh(mesh.devices.reshape(mesh.shape["section"], *split_dp(mesh)), AXES)
    placed = (
        P(None, DP, None),
        P(None, DP, None),
        P(),
        P(),
        P(),
        P("section", None, None),
        P("section", None, None),
        P("section", None, None),
    )
    return jax.shard_map(
        functools.partial(per_device, finer),
        mesh=finer,
        in_specs=placed,
        out_specs=(P("section", DP, None), P("section", DP, None), P("section", None, DP)),
        check_vma=False,
    )


def split_dp(mesh):
    count = mesh.shape["dp"]
    return (4, 4, 2) if count == 32 else (1, count, 1)
```

```python
import functools
import math

import jax
import jax.numpy as jnp
from jax import lax
from jax.experimental import pallas as pl
from jax.experimental.pallas import tpu as pltpu
from jax.sharding import Mesh
from jax.sharding import PartitionSpec as P

DP = ("dp_0", "dp_1", "dp_2")
AXES = ("section",) + DP
NORM_FLOOR = 0.1
ROWS = 32
LAG = 3
VMEM_LIMIT = 63 * 1024 * 1024
MESH = pl.DeviceIdType.MESH


def conditions(guide_bin, time_step, guide_table):
    total = guide_table.shape[1]
    half = total // 2
    frequency = jnp.exp(-math.log(10000.0) * jnp.arange(half, dtype=jnp.float32) / half)
    angle = time_step.astype(jnp.float32)[..., None] * frequency
    waves = jnp.concatenate([jnp.sin(angle), jnp.cos(angle)], axis=-1)
    bin_count = guide_table.shape[0]
    onehot = (guide_bin[..., None] == jnp.arange(bin_count, dtype=jnp.int32)).astype(jnp.float32)
    picked = jnp.einsum(
        "msb,bw->msw", onehot, guide_table.astype(jnp.float32), precision=lax.Precision.HIGHEST
    )
    return picked + 0.5 * waves


def dot_plain(left, right):
    return lax.dot_general(
        left, right, (((1,), (0,)), ((), ())), preferred_element_type=jnp.float32
    )


def dot_transposed(left, right):
    return lax.dot_general(
        left, right, (((1,), (1,)), ((), ())), preferred_element_type=jnp.float32
    )


def pipeline_kernel(
    dims,
    inputs_ref,
    out_grad_ref,
    modulation_ref,
    value_ref,
    proj_ref,
    value_out,
    proj_out,
    table_out,
    x_in,
    g_in,
    x_out,
    g_out,
    keep_mod,
    keep_val,
    keep_norm,
    keep_inv,
    keep_proj,
    own_grad,
    peer_grad,
    turned,
    peer_turned,
    table_sum,
    table_now,
    table_got,
    first_stage,
    first_got,
    second_stage,
    second_got,
    far_stage,
    far_got,
    own_sum,
    load_sem,
    fwd_send,
    fwd_recv,
    bwd_send,
    bwd_recv,
    mirror_send,
    grad_send,
    grad_recv,
    turn_send,
    turn_recv,
    first_send,
    first_recv,
    second_send,
    second_recv,
    far_send,
    far_recv,
    table_send,
    table_recv,
):
    sections, ys, zs, cores, chunks, per_micro, rows = dims
    section = lax.axis_index("section")
    y_at = lax.axis_index("dp_0")
    z_at = lax.axis_index("dp_1")
    core = lax.axis_index("dp_2")
    last = sections - 1
    half = sections // 2
    batches = chunks // per_micro
    tok_micro = per_micro * rows
    width = x_in.shape[2]
    tall = own_sum.shape[3]
    mirrored = zs - 1 - z_at
    next_z = jnp.where(section == half - 1, mirrored, z_at)
    prev_z = jnp.where(section == half, mirrored, z_at)
    next_id = (jnp.minimum(section + 1, last), y_at, next_z, core)
    prev_id = (jnp.maximum(section - 1, 0), y_at, prev_z, core)
    mirror_id = (section, y_at, mirrored, core)
    peer_id = (section, y_at, z_at, 1 - core)

    def y_id(step):
        return (section, (y_at + step + ys) % ys, z_at, core)

    def z_id(step):
        return (section, y_at, (z_at + step + zs) % zs, core)

    def remote(src, dst, send_sem, recv_sem, device_id):
        return pltpu.make_async_remote_copy(
            src_ref=src,
            dst_ref=dst,
            send_sem=send_sem,
            recv_sem=recv_sem,
            device_id=device_id,
            device_id_type=MESH,
        )

    def load(c):
        return pltpu.make_async_copy(inputs_ref.at[c], x_in.at[c], load_sem.at[c])

    def send_forward(c):
        return remote(x_out.at[c], x_in.at[c], fwd_send.at[c], fwd_recv.at[c], next_id)

    def send_backward(c):
        return remote(g_out.at[c], g_in.at[c], bwd_send.at[c], bwd_recv.at[c], prev_id)

    def send_mirror(c):
        return remote(out_grad_ref.at[c], g_in.at[c], mirror_send.at[c], bwd_recv.at[c], mirror_id)

    def share_grad(kind, c):
        at = pl.ds(pl.multiple_of(c * rows, rows), rows)
        return remote(
            own_grad.at[kind, at],
            peer_grad.at[kind, at],
            grad_send.at[kind, c],
            grad_recv.at[kind, c],
            peer_id,
        )

    def share_turned(kind):
        return remote(
            turned.at[kind, 1 - core],
            peer_turned.at[kind],
            turn_send.at[kind],
            turn_recv.at[kind],
            peer_id,
        )

    @pl.when(section == 0)
    def _():
        @pl.loop(0, chunks)
        def _(c):
            load(c).start()

    barrier = pltpu.get_barrier_semaphore()

    def greet(device_id):
        pl.semaphore_signal(barrier, inc=1, device_id=device_id, device_id_type=MESH)

    @pl.when(section < last)
    def _():
        greet(next_id)

    @pl.when(section > 0)
    def _():
        greet(prev_id)

    @pl.when(section == last)
    def _():
        greet(mirror_id)

    greet(peer_id)
    for step in range(1, ys):
        greet(y_id(step))
    for step in range(1, zs):
        greet(z_id(step))
    pl.semaphore_wait(barrier, jnp.where(section == 0, 1, 2) + ys + zs - 1)

    @pl.when(section == last)
    def _():
        @pl.loop(0, chunks)
        def _(c):
            send_mirror(c).start()

    table_sum[...] = jnp.zeros_like(table_sum)

    def forward(c):
        @pl.when(section == 0)
        def _():
            load(c).wait()

        @pl.when(section > 0)
        def _():
            send_forward(c).wait_recv()

        batch = c // per_micro
        hidden = x_in[c].astype(jnp.float32)
        centre = jnp.mean(hidden, axis=-1, keepdims=True)
        centred = hidden - centre
        spread = jnp.mean(centred * centred, axis=-1, keepdims=True)
        inverse = lax.rsqrt(spread + NORM_FLOOR)
        normed = centred * inverse
        shift = modulation_ref[batch, 0:1, :]
        scale = modulation_ref[batch, 1:2, :]
        gate = modulation_ref[batch, 2:3, :]
        modulated = (normed * scale + shift).astype(jnp.bfloat16)
        values = dot_plain(modulated, value_ref[...]).astype(jnp.bfloat16)
        projected = dot_plain(values, proj_ref[...])

        @pl.when(section < last)
        def _():
            x_out[c] = (hidden + gate * projected).astype(jnp.bfloat16)
            send_forward(c).start()

        keep_mod[c] = modulated
        keep_val[c] = values
        keep_norm[c] = normed
        keep_inv[c] = jnp.broadcast_to(inverse, (rows, 128))
        keep_proj[c] = projected

    def backward(c):
        batch = c // per_micro
        at = pl.ds(pl.multiple_of(c * rows, rows), rows)
        scale = modulation_ref[batch, 1:2, :]
        gate = modulation_ref[batch, 2:3, :]
        send_backward(c).wait_recv()
        grad_up = g_in[c].astype(jnp.float32)
        grad_proj = (gate * grad_up).astype(jnp.bfloat16)
        grad_values = dot_transposed(grad_proj, proj_ref[...]).astype(jnp.bfloat16)
        grad_mod = dot_transposed(grad_values, value_ref[...])
        normed = keep_norm[c]

        @pl.when(section > 0)
        def _():
            grad_norm = grad_mod * scale
            centre_grad = jnp.mean(grad_norm, axis=-1, keepdims=True)
            cross = jnp.mean(grad_norm * normed, axis=-1, keepdims=True)
            inverse = keep_inv[c][:, 0:1]
            grad_in = grad_up + inverse * (grad_norm - centre_grad - normed * cross)
            g_out[c] = grad_in.astype(jnp.bfloat16)
            send_backward(c).start()

        own_grad[0, at] = grad_values
        own_grad[1, at] = grad_proj
        share_grad(0, c).start()
        share_grad(1, c).start()

        def folded(value):
            return value.reshape(rows // 8, 8, width).sum(axis=0)

        table_sum[0] += folded(grad_mod)
        table_sum[1] += folded(grad_mod * normed)
        table_sum[2] += folded(grad_up * keep_proj[c])

    def turn():
        for kind, keep in ((0, keep_mod), (1, keep_val)):
            for batch in range(batches):
                part = keep[pl.ds(batch * per_micro, per_micro)].reshape(tok_micro, width)
                flipped = part.T.reshape(ys, zs, cores, tall, tok_micro)
                for z in range(zs):
                    for to in range(cores):
                        turned[kind, to, z, :, :, pl.ds(batch * tok_micro, tok_micro)] = flipped[
                            :, z, to
                        ]
            share_turned(kind).start()

    lag = LAG * (last - section)
    turn_at = jnp.where(lag >= chunks, chunks, chunks + lag)

    @pl.loop(0, chunks + LAG * last + 1)
    def _(i):
        @pl.when(i < chunks)
        def _():
            forward(i)

        @pl.when(i == turn_at)
        def _():
            turn()

        c = i - lag

        @pl.when((c >= 0) & (c < chunks))
        def _():
            backward(c)

    table_now[...] = jnp.zeros_like(table_now)
    for part in range(3):
        table_now[0, part : part + 1, :] = table_sum[part].sum(axis=0, keepdims=True)

    def share_table(stage, slot, device_id):
        return remote(
            table_now.at[stage],
            table_got.at[slot],
            table_send.at[slot],
            table_recv.at[slot],
            device_id,
        )

    table_moves = [[share_table(0, 0, peer_id)]]
    table_moves.append([share_table(1, step, y_id(step)) for step in range(1, ys)])
    table_moves.append([share_table(2, ys + step - 1, z_id(step)) for step in range(1, zs)])

    def table_step(stage):
        total = table_now[stage]
        for move in table_moves[stage]:
            move.wait_recv()
        for slot in {0: [0], 1: range(1, ys), 2: range(ys, ys + zs - 1)}[stage]:
            total = total + table_got[slot]
        table_now[stage + 1] = total
        if stage < 2:
            for move in table_moves[stage + 1]:
                move.start()

    for move in table_moves[0]:
        move.start()

    @pl.loop(0, chunks)
    def _(c):
        share_grad(0, c).wait_recv()
        share_grad(1, c).wait_recv()

    share_turned(0).wait_recv()
    share_turned(1).wait_recv()

    def z_of(seg):
        return (z_at + 2 * zs - 1 - seg) % zs

    ahead = (y_at + 1) % ys
    behind = (y_at + ys - 1) % ys
    across = (y_at + 2) % ys
    toward = (1, -1)

    def first_move(seg, kind):
        return remote(
            first_stage.at[seg, kind],
            first_got.at[seg, kind],
            first_send.at[seg, kind],
            first_recv.at[seg, kind],
            y_id(toward[kind]),
        )

    def second_move(seg, kind, way):
        return remote(
            second_stage.at[seg, kind, way],
            second_got.at[seg, kind, way],
            second_send.at[seg, kind, way],
            second_recv.at[seg, kind, way],
            y_id(toward[way]),
        )

    def far_move(seg, kind):
        return remote(
            far_stage.at[seg, kind],
            far_got.at[seg, kind],
            far_send.at[seg, kind],
            far_recv.at[seg, kind],
            z_id(-1 - seg),
        )

    def compute(seg):
        z_to = z_of(seg)
        for kind in range(2):
            left = turned[kind, core, z_to].reshape(ys * tall, -1)
            left_peer = peer_turned[kind, z_to].reshape(ys * tall, -1)
            block = dot_plain(left, own_grad[kind]) + dot_plain(left_peer, peer_grad[kind])
            own_sum[seg, kind] = block.reshape(ys, tall, width)
            first_stage[seg, kind] = own_sum[seg, kind, across].astype(jnp.bfloat16)
            first_move(seg, kind).start()

    def second(seg):
        for kind in range(2):
            for way, to in ((0, ahead), (1, behind)):
                if way != kind:
                    second_stage[seg, kind, way] = own_sum[seg, kind, to].astype(jnp.bfloat16)
                    second_move(seg, kind, way).start()
        for kind, to in ((0, ahead), (1, behind)):
            first_move(seg, kind).wait_recv()
            total = own_sum[seg, kind, to] + first_got[seg, kind].astype(jnp.float32)
            second_stage[seg, kind, kind] = total.astype(jnp.bfloat16)
            second_move(seg, kind, kind).start()

    def third(seg):
        for kind in range(2):
            total = own_sum[seg, kind, y_at]
            for way in range(2):
                second_move(seg, kind, way).wait_recv()
                total = total + second_got[seg, kind, way].astype(jnp.float32)
            if seg < zs - 1:
                far_stage[seg, kind] = total.astype(jnp.bfloat16)
                far_move(seg, kind).start()
            else:
                own_sum[seg, kind, y_at] = total

    compute(0)
    for seg in range(zs):
        if seg + 1 < zs:
            compute(seg + 1)
        second(seg)
        if seg > 0:
            third(seg - 1)
        if seg == 0:
            table_step(0)
        if seg == zs - 1:
            table_step(1)
    third(zs - 1)
    table_step(2)
    me = (y_at * zs + z_at) * cores + core
    table = table_now[3]
    mine = jnp.zeros((8, tall), jnp.float32)
    for owner in range(ys * zs * cores):
        mine = mine + jnp.where(me == owner, table[:, owner * tall : (owner + 1) * tall], 0.0)
    table_out[...] = mine[:3]
    for kind, out in ((0, value_out), (1, proj_out)):
        total = own_sum[zs - 1, kind, y_at]
        for seg in range(zs - 1):
            far_move(seg, kind).wait_recv()
            total = total + far_got[seg, kind].astype(jnp.float32)
        out[...] = total

    for seg in range(zs):
        for kind in range(2):
            first_move(seg, kind).wait_send()
            second_move(seg, kind, 0).wait_send()
            second_move(seg, kind, 1).wait_send()
            if seg < zs - 1:
                far_move(seg, kind).wait_send()
    for moves in table_moves:
        for move in moves:
            move.wait_send()
    share_turned(0).wait_send()
    share_turned(1).wait_send()

    @pl.loop(0, chunks)
    def _(c):
        share_grad(0, c).wait_send()
        share_grad(1, c).wait_send()

        @pl.when(section < last)
        def _():
            send_forward(c).wait_send()

        @pl.when(section > 0)
        def _():
            send_backward(c).wait_send()

        @pl.when(section == last)
        def _():
            send_mirror(c).wait_send()


def run_pipeline(mesh, inputs, out_grad, modulation, value_weight, proj_weight):
    batches, tok_dev, width = inputs.shape
    value_width = value_weight.shape[1]
    assert value_width == width
    rows = min(ROWS, tok_dev)
    chunks = batches * tok_dev // rows
    tokens = batches * tok_dev
    sections = mesh.shape["section"]
    ys, zs, cores = (mesh.shape[name] for name in DP)
    tall = width // (ys * zs * cores)
    dims = (sections, ys, zs, cores, chunks, tok_dev // rows, rows)
    vmem = pl.BlockSpec(memory_space=pltpu.VMEM)
    hbm = pl.BlockSpec(memory_space=pl.ANY)
    half, full = jnp.bfloat16, jnp.float32

    def sems(*shape):
        return pltpu.SemaphoreType.DMA(shape)

    return pl.pallas_call(
        functools.partial(pipeline_kernel, dims),
        out_shape=(
            jax.ShapeDtypeStruct((tall, width), full),
            jax.ShapeDtypeStruct((tall, width), full),
            jax.ShapeDtypeStruct((3, tall), full),
        ),
        in_specs=[hbm, hbm, vmem, vmem, vmem],
        out_specs=(vmem,) * 3,
        scratch_shapes=[
            pltpu.VMEM((chunks, rows, width), half),
            pltpu.VMEM((chunks, rows, width), half),
            pltpu.VMEM((chunks, rows, width), half),
            pltpu.VMEM((chunks, rows, width), half),
            pltpu.VMEM((chunks, rows, width), half),
            pltpu.VMEM((chunks, rows, width), half),
            pltpu.VMEM((chunks, rows, width), full),
            pltpu.VMEM((chunks, rows, 128), full),
            pltpu.VMEM((chunks, rows, width), full),
            pltpu.VMEM((2, tokens, width), half),
            pltpu.VMEM((2, tokens, width), half),
            pltpu.VMEM((2, cores, zs, ys, tall, tokens), half),
            pltpu.VMEM((2, zs, ys, tall, tokens), half),
            pltpu.VMEM((3, 8, width), full),
            pltpu.VMEM((4, 8, width), full),
            pltpu.VMEM((ys + zs - 1, 8, width), full),
            pltpu.VMEM((zs, 2, tall, width), half),
            pltpu.VMEM((zs, 2, tall, width), half),
            pltpu.VMEM((zs, 2, 2, tall, width), half),
            pltpu.VMEM((zs, 2, 2, tall, width), half),
            pltpu.VMEM((zs - 1, 2, tall, width), half),
            pltpu.VMEM((zs - 1, 2, tall, width), half),
            pltpu.VMEM((zs, 2, ys, tall, width), full),
            sems(chunks),
            sems(chunks),
            sems(chunks),
            sems(chunks),
            sems(chunks),
            sems(chunks),
            sems(2, chunks),
            sems(2, chunks),
            sems(2),
            sems(2),
            sems(zs, 2),
            sems(zs, 2),
            sems(zs, 2, 2),
            sems(zs, 2, 2),
            sems(zs - 1, 2),
            sems(zs - 1, 2),
            sems(ys + zs - 1),
            sems(ys + zs - 1),
        ],
        compiler_params=pltpu.CompilerParams(
            collective_id=0, has_side_effects=True, vmem_limit_bytes=VMEM_LIMIT
        ),
    )(
        inputs.reshape(chunks, rows, width),
        out_grad.reshape(chunks, rows, width),
        modulation,
        value_weight,
        proj_weight,
    )


def per_device(
    mesh,
    inputs,
    out_grad,
    guide_bin,
    time_step,
    guide_table,
    section_table,
    value_weight,
    proj_weight,
):
    batches, tok_dev, width = inputs.shape
    assert guide_bin.shape[1] == 1
    condition = conditions(guide_bin, time_step, guide_table)
    modulation = condition[:, 0] + section_table[0].reshape(-1)
    modulation = modulation.reshape(batches, 3, width)
    modulation = modulation + jnp.array([0.0, 1.0, 0.0], jnp.float32)[None, :, None]
    value_part, proj_part, table_part = run_pipeline(
        mesh, inputs, out_grad, modulation, value_weight[0], proj_weight[0]
    )
    return (value_part[None], proj_part[None], table_part[None])


def solution(mesh):
    finer = Mesh(mesh.devices.reshape(mesh.shape["section"], *split_dp(mesh)), AXES)
    placed = (
        P(None, DP, None),
        P(None, DP, None),
        P(),
        P(),
        P(),
        P("section", None, None),
        P("section", None, None),
        P("section", None, None),
    )
    return jax.shard_map(
        functools.partial(per_device, finer),
        mesh=finer,
        in_specs=placed,
        out_specs=(P("section", DP, None), P("section", DP, None), P("section", None, DP)),
        check_vma=False,
    )


def split_dp(mesh):
    count = mesh.shape["dp"]
    return (4, 4, 2) if count == 32 else (1, count, 1)
```

```python
import functools
import math

import jax
import jax.numpy as jnp
from jax import lax
from jax.experimental import pallas as pl
from jax.experimental.pallas import tpu as pltpu
from jax.sharding import Mesh
from jax.sharding import PartitionSpec as P

DP = ("dp_0", "dp_1", "dp_2")
AXES = ("section",) + DP
NORM_FLOOR = 0.1
ROWS = 32
LAG = 3
RELAY_LAG = 8
VMEM_LIMIT = 67043328
MESH = pl.DeviceIdType.MESH


def dot_plain(left, right):
    return lax.dot_general(
        left, right, (((1,), (0,)), ((), ())), preferred_element_type=jnp.float32
    )


def pipeline_kernel(
    dims,
    inputs_ref,
    out_grad_ref,
    bin_ref,
    step_ref,
    guide_ref,
    section_ref,
    value_hbm,
    proj_hbm,
    value_out,
    proj_out,
    table_out,
    x_in,
    g_in,
    x_out,
    g_out,
    value_ref,
    proj_ref,
    value_turned,
    proj_turned,
    modulation_ref,
    pool,
    keep_norm,
    keep_inv,
    keep_proj,
    own_grad,
    peer_grad,
    turned,
    peer_turned,
    table_sum,
    table_now,
    table_got,
    first_stage,
    first_got,
    second_got,
    far_stage,
    far_got,
    fresh,
    partial,
    own_sum,
    load_sem,
    weight_sem,
    fwd_send,
    fwd_recv,
    bwd_send,
    bwd_recv,
    mirror_send,
    relay_send,
    relay_recv,
    grad_send,
    grad_recv,
    turn_send,
    turn_recv,
    first_send,
    first_recv,
    second_send,
    second_recv,
    far_send,
    far_recv,
    table_send,
    table_recv,
):
    sections, ys, zs, cores, chunks, per_micro, rows = dims
    section = lax.axis_index("section")
    y_at = lax.axis_index("dp_0")
    z_at = lax.axis_index("dp_1")
    core = lax.axis_index("dp_2")
    last = sections - 1
    half = sections // 2
    batches = chunks // per_micro
    tok_micro = per_micro * rows
    width = x_in.shape[2]
    tall = own_sum.shape[2]
    tokens = chunks * rows
    mirrored = zs - 1 - z_at
    next_z = jnp.where(section == half - 1, mirrored, z_at)
    prev_z = jnp.where(section == half, mirrored, z_at)
    next_id = (jnp.minimum(section + 1, last), y_at, next_z, core)
    prev_id = (jnp.maximum(section - 1, 0), y_at, prev_z, core)
    mirror_id = (section, y_at, mirrored, core)
    peer_id = (section, y_at, z_at, 1 - core)
    inner = (z_at > 0) & (z_at < zs - 1)
    hop_out = inner & (section == half - 1)
    hop_back = inner & (section == half)
    relay_out = inner & (section == 0)
    relay_back = inner & (section == last)
    first_id = (0, y_at, z_at, core)
    last_id = (last, y_at, z_at, core)
    cross_out = (half, y_at, mirrored, core)
    cross_back = (half - 1, y_at, mirrored, core)

    def y_id(step):
        return (section, (y_at + step + ys) % ys, z_at, core)

    def z_id(step):
        return (section, y_at, (z_at + step + zs) % zs, core)

    def remote(src, dst, send_sem, recv_sem, device_id):
        return pltpu.make_async_remote_copy(
            src_ref=src,
            dst_ref=dst,
            send_sem=send_sem,
            recv_sem=recv_sem,
            device_id=device_id,
            device_id_type=MESH,
        )

    def load(c):
        return pltpu.make_async_copy(inputs_ref.at[c], x_in.at[c], load_sem.at[c])

    def send_forward(c):
        return remote(x_out.at[c], x_in.at[c], fwd_send.at[c], fwd_recv.at[c], next_id)

    def send_backward(c):
        return remote(g_out.at[c], g_in.at[c], bwd_send.at[c], bwd_recv.at[c], prev_id)

    def hop_forward(c):
        return remote(x_out.at[c], g_out.at[c], fwd_send.at[c], relay_recv.at[c], first_id)

    def hop_backward(c):
        return remote(g_out.at[c], x_out.at[c], bwd_send.at[c], relay_recv.at[c], last_id)

    def relay_forward(c):
        return remote(g_out.at[c], x_in.at[c], relay_send.at[c], fwd_recv.at[c], cross_out)

    def relay_backward(c):
        return remote(x_out.at[c], g_in.at[c], relay_send.at[c], bwd_recv.at[c], cross_back)

    def send_mirror(c):
        return remote(out_grad_ref.at[c], g_in.at[c], mirror_send.at[c], bwd_recv.at[c], mirror_id)

    def share_grad(kind, c):
        at = pl.ds(pl.multiple_of(c * rows, rows), rows)
        return remote(
            own_grad.at[kind, at],
            peer_grad.at[kind, at],
            grad_send.at[kind, c],
            grad_recv.at[kind, c],
            peer_id,
        )

    def share_turned(kind):
        return remote(
            turned.at[kind, 1 - core],
            peer_turned.at[kind],
            turn_send.at[kind],
            turn_recv.at[kind],
            peer_id,
        )

    load_value = pltpu.make_async_copy(value_hbm, value_ref, weight_sem.at[0])
    load_proj = pltpu.make_async_copy(proj_hbm, proj_ref, weight_sem.at[1])
    load_value.start()
    load_proj.start()

    @pl.when(section == 0)
    def _():
        @pl.loop(0, chunks)
        def _(c):
            load(c).start()

    barrier = pltpu.get_barrier_semaphore()

    def greet(device_id):
        pl.semaphore_signal(barrier, inc=1, device_id=device_id, device_id_type=MESH)

    @pl.when(section < last)
    def _():
        greet(next_id)

    @pl.when(section > 0)
    def _():
        greet(prev_id)

    @pl.when(section == last)
    def _():
        greet(mirror_id)

    @pl.when(relay_out)
    def _():
        greet((half - 1, y_at, z_at, core))
        greet(cross_out)

    @pl.when(hop_out)
    def _():
        greet(first_id)
        greet((last, y_at, mirrored, core))

    @pl.when(hop_back)
    def _():
        greet(last_id)
        greet((0, y_at, mirrored, core))

    @pl.when(relay_back)
    def _():
        greet((half, y_at, z_at, core))
        greet(cross_back)

    relays = relay_out | hop_out | hop_back | relay_back
    greet(peer_id)
    for step in range(1, ys):
        greet(y_id(step))
    for step in range(1, zs):
        greet(z_id(step))
    half_wave = 3 * width // 2
    row_at = lax.broadcasted_iota(jnp.int32, (8, half_wave), 0)
    lane_at = lax.broadcasted_iota(jnp.int32, (8, half_wave), 1).astype(jnp.float32)
    angle = jnp.exp(-math.log(10000.0) * lane_at / half_wave)
    bin_at = lax.broadcasted_iota(jnp.int32, (8, guide_ref.shape[0]), 1)
    bin_row = lax.broadcasted_iota(jnp.int32, (8, guide_ref.shape[0]), 0)
    step = jnp.zeros((8, half_wave), jnp.float32)
    onehot = jnp.zeros(bin_at.shape, jnp.float32)
    for batch in range(batches):
        step = jnp.where(row_at == batch, step_ref[batch, 0].astype(jnp.float32), step)
        hit = (bin_row == batch) & (bin_at == bin_ref[batch, 0])
        onehot = jnp.where(hit, 1.0, onehot)
    angle = step * angle
    picked = dot_plain(onehot.astype(jnp.bfloat16), guide_ref[...])
    modulation_ref[:, :half_wave] = picked[:, :half_wave] + 0.5 * jnp.sin(angle)
    modulation_ref[:, half_wave:] = picked[:, half_wave:] + 0.5 * jnp.cos(angle)
    for part in range(3):
        at = pl.ds(part * width, width)
        row = section_ref[part : part + 1, :]
        if part == 1:
            row = row + 1.0
        modulation_ref[:, at] = modulation_ref[:, at] + row

    def modulation(batch):
        whole = modulation_ref[pl.ds(batch, 1), :]
        return whole[:, :width], whole[:, width : 2 * width], whole[:, 2 * width :]

    pl.semaphore_wait(barrier, jnp.where(section == 0, 1, 2) + jnp.where(relays, 2, 0) + ys + zs - 1)

    @pl.when(section == last)
    def _():
        @pl.loop(0, chunks)
        def _(c):
            send_mirror(c).start()

    table_sum[...] = jnp.zeros_like(table_sum)

    def forward(c):
        @pl.when(section == 0)
        def _():
            load(c).wait()

        @pl.when(section > 0)
        def _():
            send_forward(c).wait_recv()

        batch = c // per_micro
        hidden = x_in[c].astype(jnp.float32)
        centre = jnp.mean(hidden, axis=-1, keepdims=True)
        centred = hidden - centre
        spread = jnp.mean(centred * centred, axis=-1, keepdims=True)
        inverse = lax.rsqrt(spread + NORM_FLOOR)
        normed = centred * inverse
        shift, scale, gate = modulation(batch)
        modulated = (normed * scale + shift).astype(jnp.bfloat16)
        values = dot_plain(modulated, value_ref[...]).astype(jnp.bfloat16)
        projected = dot_plain(values, proj_ref[...])

        @pl.when(section < last)
        def _():
            x_out[c] = (hidden + gate * projected).astype(jnp.bfloat16)

        @pl.when((section < last) & ~hop_out)
        def _():
            send_forward(c).start()

        @pl.when(hop_out)
        def _():
            hop_forward(c).start()

        pool[pl.ds(pl.multiple_of(c * rows, rows), rows)] = modulated
        pool[pl.ds(pl.multiple_of(tokens + c * rows, rows), rows)] = values
        keep_norm[c] = normed
        keep_inv[c] = jnp.broadcast_to(inverse, (rows, 128))
        keep_proj[c] = projected

    def backward(c):
        batch = c // per_micro
        at = pl.ds(pl.multiple_of(c * rows, rows), rows)
        unused, scale, gate = modulation(batch)
        send_backward(c).wait_recv()
        grad_up = g_in[c].astype(jnp.float32)
        grad_proj = (gate * grad_up).astype(jnp.bfloat16)
        grad_values = dot_plain(grad_proj, proj_turned[...]).astype(jnp.bfloat16)
        grad_mod = dot_plain(grad_values, value_turned[...])
        normed = keep_norm[c]

        @pl.when(section > 0)
        def _():
            grad_norm = grad_mod * scale
            centre_grad = jnp.mean(grad_norm, axis=-1, keepdims=True)
            cross = jnp.mean(grad_norm * normed, axis=-1, keepdims=True)
            inverse = keep_inv[c][:, 0:1]
            grad_in = grad_up + inverse * (grad_norm - centre_grad - normed * cross)
            g_out[c] = grad_in.astype(jnp.bfloat16)

        @pl.when((section > 0) & ~hop_back)
        def _():
            send_backward(c).start()

        @pl.when(hop_back)
        def _():
            hop_backward(c).start()

        own_grad[0, at] = grad_values
        own_grad[1, at] = grad_proj
        share_grad(0, c).start()
        share_grad(1, c).start()

        def folded(value):
            return value.reshape(rows // 8, 8, width).sum(axis=0)

        table_sum[0] += folded(grad_mod)
        table_sum[1] += folded(grad_mod * normed)
        table_sum[2] += folded(grad_up * keep_proj[c])

    def turn():
        for kind in range(2):
            for batch in range(batches):
                part = pool[pl.ds(kind * tokens + batch * tok_micro, tok_micro)]
                flipped = part.T.reshape(ys, zs, cores, tall, tok_micro)
                for z in range(zs):
                    for to in range(cores):
                        turned[kind, to, z, :, :, pl.ds(batch * tok_micro, tok_micro)] = flipped[
                            :, z, to
                        ]
            share_turned(kind).start()

    def prepare():
        tile = 256

        @pl.loop(0, width // tile)
        def _(j):
            at = pl.ds(pl.multiple_of(j * tile, tile), tile)
            value_turned[:, at] = value_ref[at, :].T
            proj_turned[:, at] = proj_ref[at, :].T

    load_value.wait()
    load_proj.wait()
    lag = jnp.where(relay_out, 2 * chunks, LAG * (last - section))
    prepare_at = jnp.where((section == 0) & (lag >= chunks), chunks, 0)
    turn_at = jnp.where(lag >= chunks, chunks, chunks + lag)

    relay_from = jnp.where(relay_out, chunks, RELAY_LAG)
    rounds = chunks + max(2 * chunks, LAG * last, RELAY_LAG) + 1

    @pl.loop(0, rounds)
    def _(i):
        @pl.when(i == prepare_at)
        def _():
            prepare()

        @pl.when(i < chunks)
        def _():
            forward(i)

        @pl.when(i == turn_at)
        def _():
            turn()

        at = i - relay_from
        within = (at >= 0) & (at < chunks)

        @pl.when(within & relay_out)
        def _():
            hop_forward(at).wait_recv()
            relay_forward(at).start()

        @pl.when(within & relay_back)
        def _():
            hop_backward(at).wait_recv()
            relay_backward(at).start()

        c = i - lag

        @pl.when((c >= 0) & (c < chunks))
        def _():
            backward(c)

    table_now[...] = jnp.zeros_like(table_now)
    for part in range(3):
        table_now[0, part : part + 1, :] = table_sum[part].sum(axis=0, keepdims=True)

    def share_table(stage, slot, device_id):
        return remote(
            table_now.at[stage],
            table_got.at[slot],
            table_send.at[slot],
            table_recv.at[slot],
            device_id,
        )

    table_moves = [[share_table(0, 0, peer_id)]]
    table_moves.append([share_table(1, step, y_id(step)) for step in range(1, ys)])
    table_moves.append([share_table(2, ys + step - 1, z_id(step)) for step in range(1, zs)])

    def table_step(stage):
        total = table_now[stage]
        for move in table_moves[stage]:
            move.wait_recv()
        for slot in {0: [0], 1: range(1, ys), 2: range(ys, ys + zs - 1)}[stage]:
            total = total + table_got[slot]
        table_now[stage + 1] = total
        if stage < 2:
            for move in table_moves[stage + 1]:
                move.start()

    for move in table_moves[0]:
        move.start()

    @pl.loop(0, chunks)
    def _(c):
        share_grad(0, c).wait_recv()
        share_grad(1, c).wait_recv()

    share_turned(0).wait_recv()
    share_turned(1).wait_recv()

    def z_of(seg):
        return (z_at + 2 * zs - 1 - seg) % zs

    ahead = (y_at + 1) % ys
    behind = (y_at + ys - 1) % ys
    across = (y_at + 2) % ys
    toward = (1, -1)

    def first_move(seg, kind):
        return remote(
            first_stage.at[seg, kind],
            first_got.at[seg, kind],
            first_send.at[seg, kind],
            first_recv.at[seg, kind],
            y_id(toward[kind]),
        )

    def second_stage(seg, kind, way):
        return pl.ds(((seg * 2 + kind) * 2 + way) * tall, tall)

    def second_move(seg, kind, way):
        return remote(
            pool.at[second_stage(seg, kind, way)],
            second_got.at[seg, kind, way],
            second_send.at[seg, kind, way],
            second_recv.at[seg, kind, way],
            y_id(toward[way]),
        )

    def far_move(seg, kind):
        return remote(
            far_stage.at[seg, kind],
            far_got.at[seg, kind],
            far_send.at[seg, kind],
            far_recv.at[seg, kind],
            z_id(-1 - seg),
        )

    def compute(seg):
        z_to = z_of(seg)
        for kind in range(2):
            left = turned[kind, core, z_to].reshape(ys * tall, -1)
            left_peer = peer_turned[kind, z_to].reshape(ys * tall, -1)
            block = dot_plain(left, own_grad[kind]) + dot_plain(left_peer, peer_grad[kind])
            fresh[...] = block.reshape(ys, tall, width)
            first_stage[seg, kind] = fresh[across].astype(jnp.bfloat16)
            first_move(seg, kind).start()
            onward, other = (ahead, behind) if kind == 0 else (behind, ahead)
            pool[second_stage(seg, kind, 1 - kind)] = fresh[other].astype(jnp.bfloat16)
            partial[seg, kind] = fresh[onward]
            own_sum[seg, kind] = fresh[y_at]

    def second(seg):
        for kind in range(2):
            second_move(seg, kind, 1 - kind).start()
        for kind in range(2):
            first_move(seg, kind).wait_recv()
            total = partial[seg, kind] + first_got[seg, kind].astype(jnp.float32)
            pool[second_stage(seg, kind, kind)] = total.astype(jnp.bfloat16)
            second_move(seg, kind, kind).start()

    def third(seg):
        for kind in range(2):
            total = own_sum[seg, kind]
            for way in range(2):
                second_move(seg, kind, way).wait_recv()
                total = total + second_got[seg, kind, way].astype(jnp.float32)
            if seg < zs - 1:
                far_stage[seg, kind] = total.astype(jnp.bfloat16)
                far_move(seg, kind).start()
            else:
                own_sum[seg, kind] = total

    compute(0)
    for seg in range(zs):
        if seg + 1 < zs:
            compute(seg + 1)
        second(seg)
        if seg > 0:
            third(seg - 1)
        if seg == 0:
            table_step(0)
        if seg == zs - 1:
            table_step(1)
    third(zs - 1)
    table_step(2)
    me = (y_at * zs + z_at) * cores + core
    table = table_now[3]
    mine = jnp.zeros((8, tall), jnp.float32)
    for owner in range(ys * zs * cores):
        mine = mine + jnp.where(me == owner, table[:, owner * tall : (owner + 1) * tall], 0.0)
    table_out[...] = mine[:3]
    for kind, out in ((0, value_out), (1, proj_out)):
        total = own_sum[zs - 1, kind]
        for seg in range(zs - 1):
            far_move(seg, kind).wait_recv()
            total = total + far_got[seg, kind].astype(jnp.float32)
        out[...] = total

    for seg in range(zs):
        for kind in range(2):
            first_move(seg, kind).wait_send()
            second_move(seg, kind, 0).wait_send()
            second_move(seg, kind, 1).wait_send()
            if seg < zs - 1:
                far_move(seg, kind).wait_send()
    for moves in table_moves:
        for move in moves:
            move.wait_send()
    share_turned(0).wait_send()
    share_turned(1).wait_send()

    @pl.loop(0, chunks)
    def _(c):
        share_grad(0, c).wait_send()
        share_grad(1, c).wait_send()

        @pl.when(section < last)
        def _():
            send_forward(c).wait_send()

        @pl.when(section > 0)
        def _():
            send_backward(c).wait_send()

        @pl.when(section == last)
        def _():
            send_mirror(c).wait_send()

        @pl.when(relay_out)
        def _():
            relay_forward(c).wait_send()

        @pl.when(relay_back)
        def _():
            relay_backward(c).wait_send()


def per_device(
    mesh,
    inputs,
    out_grad,
    guide_bin,
    time_step,
    guide_table,
    section_table,
    value_weight,
    proj_weight,
):
    batches, tok_dev, width = inputs.shape
    assert value_weight.shape[2] == width
    assert guide_bin.shape[1] == 1
    assert batches <= 8
    rows = min(ROWS, tok_dev)
    chunks = batches * tok_dev // rows
    tokens = batches * tok_dev
    sections = mesh.shape["section"]
    ys, zs, cores = (mesh.shape[name] for name in DP)
    tall = width // (ys * zs * cores)
    dims = (sections, ys, zs, cores, chunks, tok_dev // rows, rows)
    vmem = pl.BlockSpec(memory_space=pltpu.VMEM)
    smem = pl.BlockSpec(memory_space=pltpu.SMEM)
    hbm = pl.BlockSpec(memory_space=pl.ANY)
    half, full = jnp.bfloat16, jnp.float32

    def sems(*shape):
        return pltpu.SemaphoreType.DMA(shape)

    block = pltpu.VMEM((chunks, rows, width), half)
    wide = pltpu.VMEM((chunks, rows, width), full)
    square = pltpu.VMEM((width, width), half)
    value_part, proj_part, table_part = pl.pallas_call(
        functools.partial(pipeline_kernel, dims),
        out_shape=(
            jax.ShapeDtypeStruct((tall, width), full),
            jax.ShapeDtypeStruct((tall, width), full),
            jax.ShapeDtypeStruct((3, tall), full),
        ),
        in_specs=[hbm, hbm, smem, smem, vmem, vmem, hbm, hbm],
        out_specs=(vmem,) * 3,
        scratch_shapes=[
            block,
            block,
            block,
            block,
            square,
            square,
            square,
            square,
            pltpu.VMEM((8, 3 * width), full),
            pltpu.VMEM((max(2 * tokens, 4 * zs * tall), width), half),
            wide,
            pltpu.VMEM((chunks, rows, 128), full),
            wide,
            pltpu.VMEM((2, tokens, width), half),
            pltpu.VMEM((2, tokens, width), half),
            pltpu.VMEM((2, cores, zs, ys, tall, tokens), half),
            pltpu.VMEM((2, zs, ys, tall, tokens), half),
            pltpu.VMEM((3, 8, width), full),
            pltpu.VMEM((4, 8, width), full),
            pltpu.VMEM((ys + zs - 1, 8, width), full),
            pltpu.VMEM((zs, 2, tall, width), half),
            pltpu.VMEM((zs, 2, tall, width), half),
            pltpu.VMEM((zs, 2, 2, tall, width), half),
            pltpu.VMEM((zs - 1, 2, tall, width), half),
            pltpu.VMEM((zs - 1, 2, tall, width), half),
            pltpu.VMEM((ys, tall, width), full),
            pltpu.VMEM((zs, 2, tall, width), full),
            pltpu.VMEM((zs, 2, tall, width), full),
            sems(chunks),
            sems(2),
            sems(chunks),
            sems(chunks),
            sems(chunks),
            sems(chunks),
            sems(chunks),
            sems(chunks),
            sems(chunks),
            sems(2, chunks),
            sems(2, chunks),
            sems(2),
            sems(2),
            sems(zs, 2),
            sems(zs, 2),
            sems(zs, 2, 2),
            sems(zs, 2, 2),
            sems(zs - 1, 2),
            sems(zs - 1, 2),
            sems(ys + zs - 1),
            sems(ys + zs - 1),
        ],
        compiler_params=pltpu.CompilerParams(
            collective_id=0, has_side_effects=True, vmem_limit_bytes=VMEM_LIMIT
        ),
    )(
        inputs.reshape(chunks, rows, width),
        out_grad.reshape(chunks, rows, width),
        guide_bin,
        time_step,
        guide_table,
        section_table[0],
        value_weight[0],
        proj_weight[0],
    )
    return (value_part[None], proj_part[None], table_part[None])


def solution(mesh):
    finer = Mesh(mesh.devices.reshape(mesh.shape["section"], *split_dp(mesh)), AXES)
    placed = (
        P(None, DP, None),
        P(None, DP, None),
        P(),
        P(),
        P(),
        P("section", None, None),
        P("section", None, None),
        P("section", None, None),
    )
    return jax.shard_map(
        functools.partial(per_device, finer),
        mesh=finer,
        in_specs=placed,
        out_specs=(P("section", DP, None), P("section", DP, None), P("section", None, DP)),
        check_vma=False,
    )


def split_dp(mesh):
    count = mesh.shape["dp"]
    return (4, 4, 2) if count == 32 else (1, count, 1)
```

```python
import functools
import math

import jax
import jax.numpy as jnp
from jax import lax
from jax.experimental import pallas as pl
from jax.experimental.pallas import tpu as pltpu
from jax.sharding import Mesh
from jax.sharding import PartitionSpec as P

DP = ("dp_0", "dp_1", "dp_2")
AXES = ("section",) + DP
NORM_FLOOR = 0.1
ROWS = 32
LAG = 3
CROSS_LAG = 2
VMEM_LIMIT = 67043328
MESH = pl.DeviceIdType.MESH


def dot_plain(left, right):
    return lax.dot_general(
        left, right, (((1,), (0,)), ((), ())), preferred_element_type=jnp.float32
    )


def pipeline_kernel(
    dims,
    inputs_ref,
    out_grad_ref,
    bin_ref,
    step_ref,
    guide_ref,
    section_ref,
    value_hbm,
    proj_hbm,
    value_out,
    proj_out,
    table_out,
    x_in,
    g_in,
    x_out,
    g_out,
    value_ref,
    proj_ref,
    value_turned,
    proj_turned,
    modulation_ref,
    pool,
    keep_norm,
    keep_inv,
    keep_proj,
    own_grad,
    peer_grad,
    turned,
    peer_turned,
    table_sum,
    table_now,
    table_got,
    first_stage,
    first_got,
    second_got,
    far_stage,
    far_got,
    fresh,
    partial,
    own_sum,
    load_sem,
    weight_sem,
    fwd_send,
    fwd_recv,
    bwd_send,
    bwd_recv,
    mirror_send,
    grad_send,
    grad_recv,
    turn_send,
    turn_recv,
    first_send,
    first_recv,
    second_send,
    second_recv,
    far_send,
    far_recv,
    table_send,
    table_recv,
):
    sections, ys, zs, cores, chunks, per_micro, rows = dims
    section = lax.axis_index("section")
    y_at = lax.axis_index("dp_0")
    z_at = lax.axis_index("dp_1")
    core = lax.axis_index("dp_2")
    last = sections - 1
    half = sections // 2
    batches = chunks // per_micro
    tok_micro = per_micro * rows
    width = x_in.shape[2]
    tall = own_sum.shape[2]
    tokens = chunks * rows
    mirrored = zs - 1 - z_at
    next_z = jnp.where(section == half - 1, mirrored, z_at)
    prev_z = jnp.where(section == half, mirrored, z_at)
    next_id = (jnp.minimum(section + 1, last), y_at, next_z, core)
    prev_id = (jnp.maximum(section - 1, 0), y_at, prev_z, core)
    mirror_id = (section, y_at, mirrored, core)
    peer_id = (section, y_at, z_at, 1 - core)

    def y_id(step):
        return (section, (y_at + step + ys) % ys, z_at, core)

    def z_id(step):
        return (section, y_at, (z_at + step + zs) % zs, core)

    def remote(src, dst, send_sem, recv_sem, device_id):
        return pltpu.make_async_remote_copy(
            src_ref=src,
            dst_ref=dst,
            send_sem=send_sem,
            recv_sem=recv_sem,
            device_id=device_id,
            device_id_type=MESH,
        )

    def load(c):
        return pltpu.make_async_copy(inputs_ref.at[c], x_in.at[c], load_sem.at[c])

    def send_forward(c):
        return remote(x_out.at[c], x_in.at[c], fwd_send.at[c], fwd_recv.at[c], next_id)

    def send_backward(c):
        return remote(g_out.at[c], g_in.at[c], bwd_send.at[c], bwd_recv.at[c], prev_id)

    def send_mirror(c):
        return remote(out_grad_ref.at[c], g_in.at[c], mirror_send.at[c], bwd_recv.at[c], mirror_id)

    def share_grad(kind, c):
        at = pl.ds(pl.multiple_of(c * rows, rows), rows)
        return remote(
            own_grad.at[kind, at],
            peer_grad.at[kind, at],
            grad_send.at[kind, c],
            grad_recv.at[kind, c],
            peer_id,
        )

    def share_turned(kind):
        return remote(
            turned.at[kind, 1 - core],
            peer_turned.at[kind],
            turn_send.at[kind],
            turn_recv.at[kind],
            peer_id,
        )

    load_value = pltpu.make_async_copy(value_hbm, value_ref, weight_sem.at[0])
    load_proj = pltpu.make_async_copy(proj_hbm, proj_ref, weight_sem.at[1])
    load_value.start()
    load_proj.start()

    @pl.when(section == 0)
    def _():
        @pl.loop(0, chunks)
        def _(c):
            load(c).start()

    barrier = pltpu.get_barrier_semaphore()

    def greet(device_id):
        pl.semaphore_signal(barrier, inc=1, device_id=device_id, device_id_type=MESH)

    @pl.when(section < last)
    def _():
        greet(next_id)

    @pl.when(section > 0)
    def _():
        greet(prev_id)

    @pl.when(section == last)
    def _():
        greet(mirror_id)

    greet(peer_id)
    for step in range(1, ys):
        greet(y_id(step))
    for step in range(1, zs):
        greet(z_id(step))
    half_wave = 3 * width // 2
    row_at = lax.broadcasted_iota(jnp.int32, (8, half_wave), 0)
    lane_at = lax.broadcasted_iota(jnp.int32, (8, half_wave), 1).astype(jnp.float32)
    angle = jnp.exp(-math.log(10000.0) * lane_at / half_wave)
    bin_at = lax.broadcasted_iota(jnp.int32, (8, guide_ref.shape[0]), 1)
    bin_row = lax.broadcasted_iota(jnp.int32, (8, guide_ref.shape[0]), 0)
    step = jnp.zeros((8, half_wave), jnp.float32)
    onehot = jnp.zeros(bin_at.shape, jnp.float32)
    for batch in range(batches):
        step = jnp.where(row_at == batch, step_ref[batch, 0].astype(jnp.float32), step)
        hit = (bin_row == batch) & (bin_at == bin_ref[batch, 0])
        onehot = jnp.where(hit, 1.0, onehot)
    angle = step * angle
    picked = dot_plain(onehot.astype(jnp.bfloat16), guide_ref[...])
    modulation_ref[:, :half_wave] = picked[:, :half_wave] + 0.5 * jnp.sin(angle)
    modulation_ref[:, half_wave:] = picked[:, half_wave:] + 0.5 * jnp.cos(angle)
    for part in range(3):
        at = pl.ds(part * width, width)
        row = section_ref[part : part + 1, :]
        if part == 1:
            row = row + 1.0
        modulation_ref[:, at] = modulation_ref[:, at] + row

    def modulation(batch):
        whole = modulation_ref[pl.ds(batch, 1), :]
        return whole[:, :width], whole[:, width : 2 * width], whole[:, 2 * width :]

    pl.semaphore_wait(barrier, jnp.where(section == 0, 1, 2) + ys + zs - 1)

    @pl.when(section == last)
    def _():
        @pl.loop(0, chunks)
        def _(c):
            send_mirror(c).start()

    table_sum[...] = jnp.zeros_like(table_sum)

    def forward(c):
        @pl.when(section == 0)
        def _():
            load(c).wait()

        @pl.when(section > 0)
        def _():
            send_forward(c).wait_recv()

        batch = c // per_micro
        hidden = x_in[c].astype(jnp.float32)
        centre = jnp.mean(hidden, axis=-1, keepdims=True)
        centred = hidden - centre
        spread = jnp.mean(centred * centred, axis=-1, keepdims=True)
        inverse = lax.rsqrt(spread + NORM_FLOOR)
        normed = centred * inverse
        shift, scale, gate = modulation(batch)
        modulated = (normed * scale + shift).astype(jnp.bfloat16)
        values = dot_plain(modulated, value_ref[...]).astype(jnp.bfloat16)
        projected = dot_plain(values, proj_ref[...])

        @pl.when(section < last)
        def _():
            x_out[c] = (hidden + gate * projected).astype(jnp.bfloat16)
            send_forward(c).start()

        pool[pl.ds(pl.multiple_of(c * rows, rows), rows)] = modulated
        pool[pl.ds(pl.multiple_of(tokens + c * rows, rows), rows)] = values
        keep_norm[c] = normed
        keep_inv[c] = jnp.broadcast_to(inverse, (rows, 128))
        keep_proj[c] = projected

    def backward(c):
        batch = c // per_micro
        at = pl.ds(pl.multiple_of(c * rows, rows), rows)
        unused, scale, gate = modulation(batch)
        send_backward(c).wait_recv()
        grad_up = g_in[c].astype(jnp.float32)
        grad_proj = (gate * grad_up).astype(jnp.bfloat16)
        grad_values = dot_plain(grad_proj, proj_turned[...]).astype(jnp.bfloat16)
        grad_mod = dot_plain(grad_values, value_turned[...])
        normed = keep_norm[c]

        @pl.when(section > 0)
        def _():
            grad_norm = grad_mod * scale
            centre_grad = jnp.mean(grad_norm, axis=-1, keepdims=True)
            cross = jnp.mean(grad_norm * normed, axis=-1, keepdims=True)
            inverse = keep_inv[c][:, 0:1]
            grad_in = grad_up + inverse * (grad_norm - centre_grad - normed * cross)
            g_out[c] = grad_in.astype(jnp.bfloat16)
            send_backward(c).start()

        own_grad[0, at] = grad_values
        own_grad[1, at] = grad_proj
        share_grad(0, c).start()
        share_grad(1, c).start()

        def folded(value):
            return value.reshape(rows // 8, 8, width).sum(axis=0)

        table_sum[0] += folded(grad_mod)
        table_sum[1] += folded(grad_mod * normed)
        table_sum[2] += folded(grad_up * keep_proj[c])

    def turn():
        for kind in range(2):
            for batch in range(batches):
                part = pool[pl.ds(kind * tokens + batch * tok_micro, tok_micro)]
                flipped = part.T.reshape(ys, zs, cores, tall, tok_micro)
                for z in range(zs):
                    for to in range(cores):
                        turned[kind, to, z, :, :, pl.ds(batch * tok_micro, tok_micro)] = flipped[
                            :, z, to
                        ]
            share_turned(kind).start()

    def prepare():
        tile = 256

        @pl.loop(0, width // tile)
        def _(j):
            at = pl.ds(pl.multiple_of(j * tile, tile), tile)
            value_turned[:, at] = value_ref[at, :].T
            proj_turned[:, at] = proj_ref[at, :].T

    load_value.wait()
    load_proj.wait()
    lag = LAG * (last - section) + jnp.where(section < half, CROSS_LAG, 0)
    prepare_at = jnp.where((section == 0) & (lag >= chunks), chunks, 0)
    turn_at = jnp.where(lag >= chunks, chunks, chunks + lag)

    @pl.loop(0, chunks + LAG * last + CROSS_LAG + 1)
    def _(i):
        @pl.when(i == prepare_at)
        def _():
            prepare()

        @pl.when(i < chunks)
        def _():
            forward(i)

        @pl.when(i == turn_at)
        def _():
            turn()

        c = i - lag

        @pl.when((c >= 0) & (c < chunks))
        def _():
            backward(c)

    table_now[...] = jnp.zeros_like(table_now)
    for part in range(3):
        table_now[0, part : part + 1, :] = table_sum[part].sum(axis=0, keepdims=True)

    def share_table(stage, slot, device_id):
        return remote(
            table_now.at[stage],
            table_got.at[slot],
            table_send.at[slot],
            table_recv.at[slot],
            device_id,
        )

    table_moves = [[share_table(0, 0, peer_id)]]
    table_moves.append([share_table(1, step, y_id(step)) for step in range(1, ys)])
    table_moves.append([share_table(2, ys + step - 1, z_id(step)) for step in range(1, zs)])

    def table_step(stage):
        total = table_now[stage]
        for move in table_moves[stage]:
            move.wait_recv()
        for slot in {0: [0], 1: range(1, ys), 2: range(ys, ys + zs - 1)}[stage]:
            total = total + table_got[slot]
        table_now[stage + 1] = total
        if stage < 2:
            for move in table_moves[stage + 1]:
                move.start()

    for move in table_moves[0]:
        move.start()

    @pl.loop(0, chunks)
    def _(c):
        share_grad(0, c).wait_recv()
        share_grad(1, c).wait_recv()

    share_turned(0).wait_recv()
    share_turned(1).wait_recv()

    def z_of(seg):
        return (z_at + 2 * zs - 1 - seg) % zs

    ahead = (y_at + 1) % ys
    behind = (y_at + ys - 1) % ys
    across = (y_at + 2) % ys
    toward = (1, -1)

    def first_move(seg, kind):
        return remote(
            first_stage.at[seg, kind],
            first_got.at[seg, kind],
            first_send.at[seg, kind],
            first_recv.at[seg, kind],
            y_id(toward[kind]),
        )

    def second_stage(seg, kind, way):
        return pl.ds(((seg * 2 + kind) * 2 + way) * tall, tall)

    def second_move(seg, kind, way):
        return remote(
            pool.at[second_stage(seg, kind, way)],
            second_got.at[seg, kind, way],
            second_send.at[seg, kind, way],
            second_recv.at[seg, kind, way],
            y_id(toward[way]),
        )

    def far_move(seg, kind):
        return remote(
            far_stage.at[seg, kind],
            far_got.at[seg, kind],
            far_send.at[seg, kind],
            far_recv.at[seg, kind],
            z_id(-1 - seg),
        )

    def compute(seg):
        z_to = z_of(seg)
        for kind in range(2):
            left = turned[kind, core, z_to].reshape(ys * tall, -1)
            left_peer = peer_turned[kind, z_to].reshape(ys * tall, -1)
            block = dot_plain(left, own_grad[kind]) + dot_plain(left_peer, peer_grad[kind])
            fresh[...] = block.reshape(ys, tall, width)
            first_stage[seg, kind] = fresh[across].astype(jnp.bfloat16)
            first_move(seg, kind).start()
            onward, other = (ahead, behind) if kind == 0 else (behind, ahead)
            pool[second_stage(seg, kind, 1 - kind)] = fresh[other].astype(jnp.bfloat16)
            partial[seg, kind] = fresh[onward]
            own_sum[seg, kind] = fresh[y_at]

    def second(seg):
        for kind in range(2):
            second_move(seg, kind, 1 - kind).start()
        for kind in range(2):
            first_move(seg, kind).wait_recv()
            total = partial[seg, kind] + first_got[seg, kind].astype(jnp.float32)
            pool[second_stage(seg, kind, kind)] = total.astype(jnp.bfloat16)
            second_move(seg, kind, kind).start()

    def third(seg):
        for kind in range(2):
            total = own_sum[seg, kind]
            for way in range(2):
                second_move(seg, kind, way).wait_recv()
                total = total + second_got[seg, kind, way].astype(jnp.float32)
            if seg < zs - 1:
                far_stage[seg, kind] = total.astype(jnp.bfloat16)
                far_move(seg, kind).start()
            else:
                own_sum[seg, kind] = total

    compute(0)
    for seg in range(zs):
        if seg + 1 < zs:
            compute(seg + 1)
        second(seg)
        if seg > 0:
            third(seg - 1)
        if seg == 0:
            table_step(0)
        if seg == zs - 1:
            table_step(1)
    third(zs - 1)
    table_step(2)
    me = (y_at * zs + z_at) * cores + core
    table = table_now[3]
    mine = jnp.zeros((8, tall), jnp.float32)
    for owner in range(ys * zs * cores):
        mine = mine + jnp.where(me == owner, table[:, owner * tall : (owner + 1) * tall], 0.0)
    table_out[...] = mine[:3]
    for kind, out in ((0, value_out), (1, proj_out)):
        total = own_sum[zs - 1, kind]
        for seg in range(zs - 1):
            far_move(seg, kind).wait_recv()
            total = total + far_got[seg, kind].astype(jnp.float32)
        out[...] = total

    for seg in range(zs):
        for kind in range(2):
            first_move(seg, kind).wait_send()
            second_move(seg, kind, 0).wait_send()
            second_move(seg, kind, 1).wait_send()
            if seg < zs - 1:
                far_move(seg, kind).wait_send()
    for moves in table_moves:
        for move in moves:
            move.wait_send()
    share_turned(0).wait_send()
    share_turned(1).wait_send()

    @pl.loop(0, chunks)
    def _(c):
        share_grad(0, c).wait_send()
        share_grad(1, c).wait_send()

        @pl.when(section < last)
        def _():
            send_forward(c).wait_send()

        @pl.when(section > 0)
        def _():
            send_backward(c).wait_send()

        @pl.when(section == last)
        def _():
            send_mirror(c).wait_send()


def per_device(
    mesh,
    inputs,
    out_grad,
    guide_bin,
    time_step,
    guide_table,
    section_table,
    value_weight,
    proj_weight,
):
    batches, tok_dev, width = inputs.shape
    assert value_weight.shape[2] == width
    assert guide_bin.shape[1] == 1
    assert batches <= 8
    rows = min(ROWS, tok_dev)
    chunks = batches * tok_dev // rows
    tokens = batches * tok_dev
    sections = mesh.shape["section"]
    ys, zs, cores = (mesh.shape[name] for name in DP)
    tall = width // (ys * zs * cores)
    dims = (sections, ys, zs, cores, chunks, tok_dev // rows, rows)
    vmem = pl.BlockSpec(memory_space=pltpu.VMEM)
    smem = pl.BlockSpec(memory_space=pltpu.SMEM)
    hbm = pl.BlockSpec(memory_space=pl.ANY)
    half, full = jnp.bfloat16, jnp.float32

    def sems(*shape):
        return pltpu.SemaphoreType.DMA(shape)

    block = pltpu.VMEM((chunks, rows, width), half)
    wide = pltpu.VMEM((chunks, rows, width), full)
    square = pltpu.VMEM((width, width), half)
    value_part, proj_part, table_part = pl.pallas_call(
        functools.partial(pipeline_kernel, dims),
        out_shape=(
            jax.ShapeDtypeStruct((tall, width), full),
            jax.ShapeDtypeStruct((tall, width), full),
            jax.ShapeDtypeStruct((3, tall), full),
        ),
        in_specs=[hbm, hbm, smem, smem, vmem, vmem, hbm, hbm],
        out_specs=(vmem,) * 3,
        scratch_shapes=[
            block,
            block,
            block,
            block,
            square,
            square,
            square,
            square,
            pltpu.VMEM((8, 3 * width), full),
            pltpu.VMEM((max(2 * tokens, 4 * zs * tall), width), half),
            wide,
            pltpu.VMEM((chunks, rows, 128), full),
            wide,
            pltpu.VMEM((2, tokens, width), half),
            pltpu.VMEM((2, tokens, width), half),
            pltpu.VMEM((2, cores, zs, ys, tall, tokens), half),
            pltpu.VMEM((2, zs, ys, tall, tokens), half),
            pltpu.VMEM((3, 8, width), full),
            pltpu.VMEM((4, 8, width), full),
            pltpu.VMEM((ys + zs - 1, 8, width), full),
            pltpu.VMEM((zs, 2, tall, width), half),
            pltpu.VMEM((zs, 2, tall, width), half),
            pltpu.VMEM((zs, 2, 2, tall, width), half),
            pltpu.VMEM((zs - 1, 2, tall, width), half),
            pltpu.VMEM((zs - 1, 2, tall, width), half),
            pltpu.VMEM((ys, tall, width), full),
            pltpu.VMEM((zs, 2, tall, width), full),
            pltpu.VMEM((zs, 2, tall, width), full),
            sems(chunks),
            sems(2),
            sems(chunks),
            sems(chunks),
            sems(chunks),
            sems(chunks),
            sems(chunks),
            sems(2, chunks),
            sems(2, chunks),
            sems(2),
            sems(2),
            sems(zs, 2),
            sems(zs, 2),
            sems(zs, 2, 2),
            sems(zs, 2, 2),
            sems(zs - 1, 2),
            sems(zs - 1, 2),
            sems(ys + zs - 1),
            sems(ys + zs - 1),
        ],
        compiler_params=pltpu.CompilerParams(
            collective_id=0, has_side_effects=True, vmem_limit_bytes=VMEM_LIMIT
        ),
    )(
        inputs.reshape(chunks, rows, width),
        out_grad.reshape(chunks, rows, width),
        guide_bin,
        time_step,
        guide_table,
        section_table[0],
        value_weight[0],
        proj_weight[0],
    )
    return (value_part[None], proj_part[None], table_part[None])


def solution(mesh):
    finer = Mesh(mesh.devices.reshape(mesh.shape["section"], *split_dp(mesh)), AXES)
    placed = (
        P(None, DP, None),
        P(None, DP, None),
        P(),
        P(),
        P(),
        P("section", None, None),
        P("section", None, None),
        P("section", None, None),
    )
    return jax.shard_map(
        functools.partial(per_device, finer),
        mesh=finer,
        in_specs=placed,
        out_specs=(P("section", DP, None), P("section", DP, None), P("section", None, DP)),
        check_vma=False,
    )


def split_dp(mesh):
    count = mesh.shape["dp"]
    return (4, 4, 2) if count == 32 else (1, count, 1)
```

```python
import functools
import math

import jax
import jax.numpy as jnp
from jax import lax
from jax.experimental import pallas as pl
from jax.experimental.pallas import tpu as pltpu
from jax.sharding import Mesh
from jax.sharding import PartitionSpec as P

DP = ("dp_0", "dp_1", "dp_2")
AXES = ("section",) + DP
NORM_FLOOR = 0.1
ROWS = 32
LAG = 3
CROSS_LAG = 4
RELAY_LAG = 8
VMEM_LIMIT = 67043328
MESH = pl.DeviceIdType.MESH


def dot_plain(left, right):
    return lax.dot_general(
        left, right, (((1,), (0,)), ((), ())), preferred_element_type=jnp.float32
    )


def pipeline_kernel(
    dims,
    inputs_ref,
    out_grad_ref,
    bin_ref,
    step_ref,
    guide_ref,
    section_ref,
    value_hbm,
    proj_hbm,
    value_out,
    proj_out,
    table_out,
    x_in,
    g_in,
    x_out,
    g_out,
    value_ref,
    proj_ref,
    value_turned,
    proj_turned,
    modulation_ref,
    pool,
    keep_norm,
    keep_inv,
    keep_proj,
    own_grad,
    peer_grad,
    turned,
    peer_turned,
    table_sum,
    table_now,
    table_got,
    first_stage,
    first_got,
    second_got,
    far_stage,
    far_got,
    fresh,
    partial,
    own_sum,
    load_sem,
    weight_sem,
    fwd_send,
    fwd_recv,
    bwd_send,
    bwd_recv,
    mirror_send,
    relay_send,
    relay_recv,
    grad_send,
    grad_recv,
    turn_send,
    turn_recv,
    first_send,
    first_recv,
    second_send,
    second_recv,
    far_send,
    far_recv,
    table_send,
    table_recv,
):
    sections, ys, zs, cores, chunks, per_micro, rows = dims
    section = lax.axis_index("section")
    y_at = lax.axis_index("dp_0")
    z_at = lax.axis_index("dp_1")
    core = lax.axis_index("dp_2")
    last = sections - 1
    half = sections // 2
    batches = chunks // per_micro
    tok_micro = per_micro * rows
    width = x_in.shape[2]
    tall = own_sum.shape[2]
    tokens = chunks * rows
    mirrored = zs - 1 - z_at
    next_z = jnp.where(section == half - 1, mirrored, z_at)
    prev_z = jnp.where(section == half, mirrored, z_at)
    next_id = (jnp.minimum(section + 1, last), y_at, next_z, core)
    prev_id = (jnp.maximum(section - 1, 0), y_at, prev_z, core)
    mirror_id = (section, y_at, mirrored, core)
    peer_id = (section, y_at, z_at, 1 - core)
    inner = (z_at > 0) & (z_at < zs - 1)
    hop_out = inner & (section == half - 1)
    hop_back = inner & (section == half)
    relay_out = inner & (section == 0)
    relay_back = inner & (section == last)
    first_id = (0, y_at, z_at, core)
    last_id = (last, y_at, z_at, core)
    cross_out = (half, y_at, mirrored, core)
    cross_back = (half - 1, y_at, mirrored, core)

    def y_id(step):
        return (section, (y_at + step + ys) % ys, z_at, core)

    def z_id(step):
        return (section, y_at, (z_at + step + zs) % zs, core)

    def remote(src, dst, send_sem, recv_sem, device_id):
        return pltpu.make_async_remote_copy(
            src_ref=src,
            dst_ref=dst,
            send_sem=send_sem,
            recv_sem=recv_sem,
            device_id=device_id,
            device_id_type=MESH,
        )

    def load(c):
        return pltpu.make_async_copy(inputs_ref.at[c], x_in.at[c], load_sem.at[c])

    def send_forward(c):
        return remote(x_out.at[c], x_in.at[c], fwd_send.at[c], fwd_recv.at[c], next_id)

    def send_backward(c):
        return remote(g_out.at[c], g_in.at[c], bwd_send.at[c], bwd_recv.at[c], prev_id)

    def hop_forward(c):
        return remote(x_out.at[c], g_out.at[c], fwd_send.at[c], relay_recv.at[c], first_id)

    def hop_backward(c):
        return remote(g_out.at[c], x_out.at[c], bwd_send.at[c], relay_recv.at[c], last_id)

    def relay_forward(c):
        return remote(g_out.at[c], x_in.at[c], relay_send.at[c], fwd_recv.at[c], cross_out)

    def relay_backward(c):
        return remote(x_out.at[c], g_in.at[c], relay_send.at[c], bwd_recv.at[c], cross_back)

    def send_mirror(c):
        return remote(out_grad_ref.at[c], g_in.at[c], mirror_send.at[c], bwd_recv.at[c], mirror_id)

    def share_grad(kind, c):
        at = pl.ds(pl.multiple_of(c * rows, rows), rows)
        return remote(
            own_grad.at[kind, at],
            peer_grad.at[kind, at],
            grad_send.at[kind, c],
            grad_recv.at[kind, c],
            peer_id,
        )

    def share_turned(kind):
        return remote(
            turned.at[kind, 1 - core],
            peer_turned.at[kind],
            turn_send.at[kind],
            turn_recv.at[kind],
            peer_id,
        )

    load_value = pltpu.make_async_copy(value_hbm, value_ref, weight_sem.at[0])
    load_proj = pltpu.make_async_copy(proj_hbm, proj_ref, weight_sem.at[1])
    load_value.start()
    load_proj.start()

    @pl.when(section == 0)
    def _():
        @pl.loop(0, chunks)
        def _(c):
            load(c).start()

    barrier = pltpu.get_barrier_semaphore()

    def greet(device_id):
        pl.semaphore_signal(barrier, inc=1, device_id=device_id, device_id_type=MESH)

    @pl.when(section < last)
    def _():
        greet(next_id)

    @pl.when(section > 0)
    def _():
        greet(prev_id)

    @pl.when(section == last)
    def _():
        greet(mirror_id)

    @pl.when(relay_out)
    def _():
        greet((half - 1, y_at, z_at, core))
        greet(cross_out)

    @pl.when(hop_out)
    def _():
        greet(first_id)
        greet((last, y_at, mirrored, core))

    @pl.when(hop_back)
    def _():
        greet(last_id)
        greet((0, y_at, mirrored, core))

    @pl.when(relay_back)
    def _():
        greet((half, y_at, z_at, core))
        greet(cross_back)

    relays = relay_out | hop_out | hop_back | relay_back
    greet(peer_id)
    for step in range(1, ys):
        greet(y_id(step))
    for step in range(1, zs):
        greet(z_id(step))
    half_wave = 3 * width // 2
    row_at = lax.broadcasted_iota(jnp.int32, (8, half_wave), 0)
    lane_at = lax.broadcasted_iota(jnp.int32, (8, half_wave), 1).astype(jnp.float32)
    angle = jnp.exp(-math.log(10000.0) * lane_at / half_wave)
    bin_at = lax.broadcasted_iota(jnp.int32, (8, guide_ref.shape[0]), 1)
    bin_row = lax.broadcasted_iota(jnp.int32, (8, guide_ref.shape[0]), 0)
    step = jnp.zeros((8, half_wave), jnp.float32)
    onehot = jnp.zeros(bin_at.shape, jnp.float32)
    for batch in range(batches):
        step = jnp.where(row_at == batch, step_ref[batch, 0].astype(jnp.float32), step)
        hit = (bin_row == batch) & (bin_at == bin_ref[batch, 0])
        onehot = jnp.where(hit, 1.0, onehot)
    angle = step * angle
    picked = dot_plain(onehot.astype(jnp.bfloat16), guide_ref[...])
    modulation_ref[:, :half_wave] = picked[:, :half_wave] + 0.5 * jnp.sin(angle)
    modulation_ref[:, half_wave:] = picked[:, half_wave:] + 0.5 * jnp.cos(angle)
    for part in range(3):
        at = pl.ds(part * width, width)
        row = section_ref[part : part + 1, :]
        if part == 1:
            row = row + 1.0
        modulation_ref[:, at] = modulation_ref[:, at] + row

    def modulation(batch):
        whole = modulation_ref[pl.ds(batch, 1), :]
        return whole[:, :width], whole[:, width : 2 * width], whole[:, 2 * width :]

    pl.semaphore_wait(barrier, jnp.where(section == 0, 1, 2) + jnp.where(relays, 2, 0) + ys + zs - 1)

    @pl.when(section == last)
    def _():
        @pl.loop(0, chunks)
        def _(c):
            send_mirror(c).start()

    table_sum[...] = jnp.zeros_like(table_sum)

    def forward(c):
        @pl.when(section == 0)
        def _():
            load(c).wait()

        @pl.when(section > 0)
        def _():
            send_forward(c).wait_recv()

        batch = c // per_micro
        hidden = x_in[c].astype(jnp.float32)
        centre = jnp.mean(hidden, axis=-1, keepdims=True)
        centred = hidden - centre
        spread = jnp.mean(centred * centred, axis=-1, keepdims=True)
        inverse = lax.rsqrt(spread + NORM_FLOOR)
        normed = centred * inverse
        shift, scale, gate = modulation(batch)
        modulated = (normed * scale + shift).astype(jnp.bfloat16)
        values = dot_plain(modulated, value_ref[...]).astype(jnp.bfloat16)
        projected = dot_plain(values, proj_ref[...])

        @pl.when(section < last)
        def _():
            x_out[c] = (hidden + gate * projected).astype(jnp.bfloat16)

        @pl.when((section < last) & ~hop_out)
        def _():
            send_forward(c).start()

        @pl.when(hop_out)
        def _():
            hop_forward(c).start()

        pool[pl.ds(pl.multiple_of(c * rows, rows), rows)] = modulated
        pool[pl.ds(pl.multiple_of(tokens + c * rows, rows), rows)] = values
        keep_norm[c] = normed
        keep_inv[c] = jnp.broadcast_to(inverse, (rows, 128))
        keep_proj[c] = projected

    def backward(c):
        batch = c // per_micro
        at = pl.ds(pl.multiple_of(c * rows, rows), rows)
        unused, scale, gate = modulation(batch)
        send_backward(c).wait_recv()
        grad_up = g_in[c].astype(jnp.float32)
        grad_proj = (gate * grad_up).astype(jnp.bfloat16)
        grad_values = dot_plain(grad_proj, proj_turned[...]).astype(jnp.bfloat16)
        grad_mod = dot_plain(grad_values, value_turned[...])
        normed = keep_norm[c]

        @pl.when(section > 0)
        def _():
            grad_norm = grad_mod * scale
            centre_grad = jnp.mean(grad_norm, axis=-1, keepdims=True)
            cross = jnp.mean(grad_norm * normed, axis=-1, keepdims=True)
            inverse = keep_inv[c][:, 0:1]
            grad_in = grad_up + inverse * (grad_norm - centre_grad - normed * cross)
            g_out[c] = grad_in.astype(jnp.bfloat16)

        @pl.when((section > 0) & ~hop_back)
        def _():
            send_backward(c).start()

        @pl.when(hop_back)
        def _():
            hop_backward(c).start()

        own_grad[0, at] = grad_values
        own_grad[1, at] = grad_proj
        share_grad(0, c).start()
        share_grad(1, c).start()

        def folded(value):
            return value.reshape(rows // 8, 8, width).sum(axis=0)

        table_sum[0] += folded(grad_mod)
        table_sum[1] += folded(grad_mod * normed)
        table_sum[2] += folded(grad_up * keep_proj[c])

    def turn():
        for kind in range(2):
            for batch in range(batches):
                part = pool[pl.ds(kind * tokens + batch * tok_micro, tok_micro)]
                flipped = part.T.reshape(ys, zs, cores, tall, tok_micro)
                for z in range(zs):
                    for to in range(cores):
                        turned[kind, to, z, :, :, pl.ds(batch * tok_micro, tok_micro)] = flipped[
                            :, z, to
                        ]
            share_turned(kind).start()

    def prepare():
        tile = 256

        @pl.loop(0, width // tile)
        def _(j):
            at = pl.ds(pl.multiple_of(j * tile, tile), tile)
            value_turned[:, at] = value_ref[at, :].T
            proj_turned[:, at] = proj_ref[at, :].T

    load_value.wait()
    load_proj.wait()
    lag = LAG * (last - section) + jnp.where(section < half, CROSS_LAG, 0)
    lag = jnp.where(relay_out, 2 * chunks, lag)
    prepare_at = jnp.where((section == 0) & (lag >= chunks), chunks, 0)
    turn_at = jnp.where(lag >= chunks, chunks, chunks + lag)

    relay_from = jnp.where(relay_out, chunks, RELAY_LAG)
    rounds = chunks + max(2 * chunks, LAG * last + CROSS_LAG, RELAY_LAG) + 1

    @pl.loop(0, rounds)
    def _(i):
        @pl.when(i == prepare_at)
        def _():
            prepare()

        @pl.when(i < chunks)
        def _():
            forward(i)

        @pl.when(i == turn_at)
        def _():
            turn()

        at = i - relay_from
        within = (at >= 0) & (at < chunks)

        @pl.when(within & relay_out)
        def _():
            hop_forward(at).wait_recv()
            relay_forward(at).start()

        @pl.when(within & relay_back)
        def _():
            hop_backward(at).wait_recv()
            relay_backward(at).start()

        c = i - lag

        @pl.when((c >= 0) & (c < chunks))
        def _():
            backward(c)

    table_now[...] = jnp.zeros_like(table_now)
    for part in range(3):
        table_now[0, part : part + 1, :] = table_sum[part].sum(axis=0, keepdims=True)

    def share_table(stage, slot, device_id):
        return remote(
            table_now.at[stage],
            table_got.at[slot],
            table_send.at[slot],
            table_recv.at[slot],
            device_id,
        )

    table_moves = [[share_table(0, 0, peer_id)]]
    table_moves.append([share_table(1, step, y_id(step)) for step in range(1, ys)])
    table_moves.append([share_table(2, ys + step - 1, z_id(step)) for step in range(1, zs)])

    def table_step(stage):
        total = table_now[stage]
        for move in table_moves[stage]:
            move.wait_recv()
        for slot in {0: [0], 1: range(1, ys), 2: range(ys, ys + zs - 1)}[stage]:
            total = total + table_got[slot]
        table_now[stage + 1] = total
        if stage < 2:
            for move in table_moves[stage + 1]:
                move.start()

    for move in table_moves[0]:
        move.start()

    @pl.loop(0, chunks)
    def _(c):
        share_grad(0, c).wait_recv()
        share_grad(1, c).wait_recv()

    share_turned(0).wait_recv()
    share_turned(1).wait_recv()

    def z_of(seg):
        return (z_at + 2 * zs - 1 - seg) % zs

    ahead = (y_at + 1) % ys
    behind = (y_at + ys - 1) % ys
    across = (y_at + 2) % ys
    toward = (1, -1)

    def first_move(seg, kind):
        return remote(
            first_stage.at[seg, kind],
            first_got.at[seg, kind],
            first_send.at[seg, kind],
            first_recv.at[seg, kind],
            y_id(toward[kind]),
        )

    def second_stage(seg, kind, way):
        return pl.ds(((seg * 2 + kind) * 2 + way) * tall, tall)

    def second_move(seg, kind, way):
        return remote(
            pool.at[second_stage(seg, kind, way)],
            second_got.at[seg, kind, way],
            second_send.at[seg, kind, way],
            second_recv.at[seg, kind, way],
            y_id(toward[way]),
        )

    def far_move(seg, kind):
        return remote(
            far_stage.at[seg, kind],
            far_got.at[seg, kind],
            far_send.at[seg, kind],
            far_recv.at[seg, kind],
            z_id(-1 - seg),
        )

    def compute(seg):
        z_to = z_of(seg)
        for kind in range(2):
            left = turned[kind, core, z_to].reshape(ys * tall, -1)
            left_peer = peer_turned[kind, z_to].reshape(ys * tall, -1)
            block = dot_plain(left, own_grad[kind]) + dot_plain(left_peer, peer_grad[kind])
            fresh[...] = block.reshape(ys, tall, width)
            first_stage[seg, kind] = fresh[across].astype(jnp.bfloat16)
            first_move(seg, kind).start()
            onward, other = (ahead, behind) if kind == 0 else (behind, ahead)
            pool[second_stage(seg, kind, 1 - kind)] = fresh[other].astype(jnp.bfloat16)
            partial[seg, kind] = fresh[onward]
            own_sum[seg, kind] = fresh[y_at]

    def second(seg):
        for kind in range(2):
            second_move(seg, kind, 1 - kind).start()
        for kind in range(2):
            first_move(seg, kind).wait_recv()
            total = partial[seg, kind] + first_got[seg, kind].astype(jnp.float32)
            pool[second_stage(seg, kind, kind)] = total.astype(jnp.bfloat16)
            second_move(seg, kind, kind).start()

    def third(seg):
        for kind in range(2):
            total = own_sum[seg, kind]
            for way in range(2):
                second_move(seg, kind, way).wait_recv()
                total = total + second_got[seg, kind, way].astype(jnp.float32)
            if seg < zs - 1:
                far_stage[seg, kind] = total.astype(jnp.bfloat16)
                far_move(seg, kind).start()
            else:
                own_sum[seg, kind] = total

    compute(0)
    for seg in range(zs):
        if seg + 1 < zs:
            compute(seg + 1)
        second(seg)
        if seg > 0:
            third(seg - 1)
        if seg == 0:
            table_step(0)
        if seg == zs - 1:
            table_step(1)
    third(zs - 1)
    table_step(2)
    me = (y_at * zs + z_at) * cores + core
    table = table_now[3]
    mine = jnp.zeros((8, tall), jnp.float32)
    for owner in range(ys * zs * cores):
        mine = mine + jnp.where(me == owner, table[:, owner * tall : (owner + 1) * tall], 0.0)
    table_out[...] = mine[:3]
    for kind, out in ((0, value_out), (1, proj_out)):
        total = own_sum[zs - 1, kind]
        for seg in range(zs - 1):
            far_move(seg, kind).wait_recv()
            total = total + far_got[seg, kind].astype(jnp.float32)
        out[...] = total

    for seg in range(zs):
        for kind in range(2):
            first_move(seg, kind).wait_send()
            second_move(seg, kind, 0).wait_send()
            second_move(seg, kind, 1).wait_send()
            if seg < zs - 1:
                far_move(seg, kind).wait_send()
    for moves in table_moves:
        for move in moves:
            move.wait_send()
    share_turned(0).wait_send()
    share_turned(1).wait_send()

    @pl.loop(0, chunks)
    def _(c):
        share_grad(0, c).wait_send()
        share_grad(1, c).wait_send()

        @pl.when(section < last)
        def _():
            send_forward(c).wait_send()

        @pl.when(section > 0)
        def _():
            send_backward(c).wait_send()

        @pl.when(section == last)
        def _():
            send_mirror(c).wait_send()

        @pl.when(relay_out)
        def _():
            relay_forward(c).wait_send()

        @pl.when(relay_back)
        def _():
            relay_backward(c).wait_send()


def per_device(
    mesh,
    inputs,
    out_grad,
    guide_bin,
    time_step,
    guide_table,
    section_table,
    value_weight,
    proj_weight,
):
    batches, tok_dev, width = inputs.shape
    assert value_weight.shape[2] == width
    assert guide_bin.shape[1] == 1
    assert batches <= 8
    rows = min(ROWS, tok_dev)
    chunks = batches * tok_dev // rows
    tokens = batches * tok_dev
    sections = mesh.shape["section"]
    ys, zs, cores = (mesh.shape[name] for name in DP)
    tall = width // (ys * zs * cores)
    dims = (sections, ys, zs, cores, chunks, tok_dev // rows, rows)
    vmem = pl.BlockSpec(memory_space=pltpu.VMEM)
    smem = pl.BlockSpec(memory_space=pltpu.SMEM)
    hbm = pl.BlockSpec(memory_space=pl.ANY)
    half, full = jnp.bfloat16, jnp.float32

    def sems(*shape):
        return pltpu.SemaphoreType.DMA(shape)

    block = pltpu.VMEM((chunks, rows, width), half)
    wide = pltpu.VMEM((chunks, rows, width), full)
    square = pltpu.VMEM((width, width), half)
    value_part, proj_part, table_part = pl.pallas_call(
        functools.partial(pipeline_kernel, dims),
        out_shape=(
            jax.ShapeDtypeStruct((tall, width), full),
            jax.ShapeDtypeStruct((tall, width), full),
            jax.ShapeDtypeStruct((3, tall), full),
        ),
        in_specs=[hbm, hbm, smem, smem, vmem, vmem, hbm, hbm],
        out_specs=(vmem,) * 3,
        scratch_shapes=[
            block,
            block,
            block,
            block,
            square,
            square,
            square,
            square,
            pltpu.VMEM((8, 3 * width), full),
            pltpu.VMEM((max(2 * tokens, 4 * zs * tall), width), half),
            wide,
            pltpu.VMEM((chunks, rows, 128), full),
            wide,
            pltpu.VMEM((2, tokens, width), half),
            pltpu.VMEM((2, tokens, width), half),
            pltpu.VMEM((2, cores, zs, ys, tall, tokens), half),
            pltpu.VMEM((2, zs, ys, tall, tokens), half),
            pltpu.VMEM((3, 8, width), full),
            pltpu.VMEM((4, 8, width), full),
            pltpu.VMEM((ys + zs - 1, 8, width), full),
            pltpu.VMEM((zs, 2, tall, width), half),
            pltpu.VMEM((zs, 2, tall, width), half),
            pltpu.VMEM((zs, 2, 2, tall, width), half),
            pltpu.VMEM((zs - 1, 2, tall, width), half),
            pltpu.VMEM((zs - 1, 2, tall, width), half),
            pltpu.VMEM((ys, tall, width), full),
            pltpu.VMEM((zs, 2, tall, width), full),
            pltpu.VMEM((zs, 2, tall, width), full),
            sems(chunks),
            sems(2),
            sems(chunks),
            sems(chunks),
            sems(chunks),
            sems(chunks),
            sems(chunks),
            sems(chunks),
            sems(chunks),
            sems(2, chunks),
            sems(2, chunks),
            sems(2),
            sems(2),
            sems(zs, 2),
            sems(zs, 2),
            sems(zs, 2, 2),
            sems(zs, 2, 2),
            sems(zs - 1, 2),
            sems(zs - 1, 2),
            sems(ys + zs - 1),
            sems(ys + zs - 1),
        ],
        compiler_params=pltpu.CompilerParams(
            collective_id=0, has_side_effects=True, vmem_limit_bytes=VMEM_LIMIT
        ),
    )(
        inputs.reshape(chunks, rows, width),
        out_grad.reshape(chunks, rows, width),
        guide_bin,
        time_step,
        guide_table,
        section_table[0],
        value_weight[0],
        proj_weight[0],
    )
    return (value_part[None], proj_part[None], table_part[None])


def solution(mesh):
    finer = Mesh(mesh.devices.reshape(mesh.shape["section"], *split_dp(mesh)), AXES)
    placed = (
        P(None, DP, None),
        P(None, DP, None),
        P(),
        P(),
        P(),
        P("section", None, None),
        P("section", None, None),
        P("section", None, None),
    )
    return jax.shard_map(
        functools.partial(per_device, finer),
        mesh=finer,
        in_specs=placed,
        out_specs=(P("section", DP, None), P("section", DP, None), P("section", None, DP)),
        check_vma=False,
    )


def split_dp(mesh):
    count = mesh.shape["dp"]
    return (4, 4, 2) if count == 32 else (1, count, 1)
```
